32 devices in a mesh: dp: 4 (over x, core), ctx: 8 (over z, y).
Axes of the slice: x: 2, y: 2, z: 4, core: 2. Of those that a mesh axis runs over, the one named last changes fastest.
Arguments:
- grad_output: bfloat16 [4, 2048, 1024], P('dp', None, 'ctx'), may hold values from -6 to 6
- post_gate: bfloat16 [4, 2048, 1024], P('dp', None, 'ctx'), may hold values from -6 to 6
- pre_gate: bfloat16 [4, 2048, 1024], P('dp', None, 'ctx'), may hold values from -6 to 6
- value_branch: bfloat16 [4, 2048, 1024], P('dp', None, 'ctx'), may hold values from -6 to 6
- long_filter: float32 [2048, 1024], P('ctx'), may hold values from -0.1875 to 0.1875
- skip_weight: float32 [2048], replicated, may hold values from -3 to 3
Outputs:
- grad_pre_gate: bfloat16 [4, 2048, 1024], P('dp', None, 'ctx')
- grad_value_branch: bfloat16 [4, 2048, 1024], P('dp', None, 'ctx')
- grad_long_filter: float32 [2048, 1024], P('ctx', 'dp')
The draws below stay inside these ranges and needn't reach their ends.
All inputs are finite; a program needn't handle non-finite values.
Results may differ from the reference program's by a relative error of at most 0.0095.
Values may be sent and summed in bfloat16 or wider, within the bound.
No kernel may reach another device: no remote copies, remote signals or barrier semaphores. Data moves between devices by JAX's collectives and lax.ppermute only.
A program may use at most 64 MiB of HBM per device.

```python
import math
import jax
import jax.numpy as jnp
from jax import lax

C = 2048
SEQ_LEN = 1024
SEQS = 4
TOKENS = 4096


def shard_levels(key, shape, cuts, low, largest):
    def one(dim, blocks):
        draws = jax.random.uniform(jax.random.fold_in(jax.random.fold_in(key, 6), dim), (blocks,), jnp.float32, low / len(cuts), largest / len(cuts))
        return jnp.repeat(jnp.exp(draws), shape[dim] // blocks).reshape((-1,) + (1,) * (len(shape) - dim - 1))

    factor_of = one(*cuts[0])
    for cut in cuts[1:]:
        factor_of = factor_of * one(*cut)
    return factor_of


def bell_draw(own_key, shape, width, bound, split=(), held_as=jnp.bfloat16):
    values = width * jax.random.normal(own_key, shape, jnp.float32)
    if split:
        values = values * shard_levels(own_key, shape, split, -0.22, 0.18)
    return jnp.clip(values, -bound, bound).astype(held_as)


def setup_inputs(seed: int = 0) -> dict:
    arg_keys = jax.random.split(jax.random.key(seed), 7)
    grad_output = bell_draw(arg_keys[0], (SEQS, C, SEQ_LEN), 1.0, 6.0, ((0, 4), (2, 8)))
    post_gate = bell_draw(arg_keys[1], (SEQS, C, SEQ_LEN), 1.0, 6.0, ((0, 4), (2, 8)))
    pre_gate = bell_draw(arg_keys[2], (SEQS, C, SEQ_LEN), 1.0, 6.0, ((0, 4), (2, 8)))
    value_branch = bell_draw(arg_keys[3], (SEQS, C, SEQ_LEN), 1.0, 6.0, ((0, 4), (2, 8)))
    long_filter = bell_draw(arg_keys[4], (C, SEQ_LEN), SEQ_LEN ** -0.5, 0.1875, ((0, 8),), jnp.float32)
    skip_weight = bell_draw(arg_keys[5], (C,), 1.0, 3.0, (), jnp.float32)
    return dict(grad_output=grad_output, post_gate=post_gate, pre_gate=pre_gate, value_branch=value_branch, long_filter=long_filter, skip_weight=skip_weight)


def reference(grad_output, post_gate, pre_gate, value_branch, long_filter, skip_weight):
    gated = (grad_output.astype(jnp.float32) * post_gate.astype(jnp.float32)).astype(jnp.bfloat16)
    saved = (pre_gate.astype(jnp.float32) * value_branch.astype(jnp.float32)).astype(jnp.bfloat16)
    length = long_filter.shape[1]
    padded = 2 * length

    def per_channel(operands):
        grad_rows, saved_rows, filter_row = operands
        grad_spec = jnp.fft.rfft(grad_rows.astype(jnp.float32), n=padded, axis=-1)
        saved_spec = jnp.fft.rfft(saved_rows.astype(jnp.float32), n=padded, axis=-1)
        filter_spec = jnp.fft.rfft(filter_row, n=padded, axis=-1)
        correlated = jnp.fft.irfft(jnp.conj(filter_spec)[None, :] * grad_spec, n=padded, axis=-1)[:, :length]
        filter_terms = jnp.fft.irfft(grad_spec * jnp.conj(saved_spec), n=padded, axis=-1)[:, :length]
        return (correlated.astype(jnp.bfloat16), lax.optimization_barrier(jnp.sum(filter_terms, axis=0)))
    correlation, filter_sum = lax.map(per_channel, (jnp.swapaxes(gated, 0, 1), jnp.swapaxes(saved, 0, 1), long_filter))
    correlation = jnp.swapaxes(correlation, 0, 1)
    summed = correlation.astype(jnp.float32) + skip_weight[None, :, None] * gated.astype(jnp.float32)
    grad_pre_gate = (summed * value_branch.astype(jnp.float32)).astype(jnp.bfloat16)
    grad_value_branch = (summed * pre_gate.astype(jnp.float32)).astype(jnp.bfloat16)
    grad_long_filter = filter_sum * (1.0 / math.sqrt(TOKENS))
    return (grad_pre_gate, grad_value_branch, grad_long_filter)
```

```python
import math

import jax
import jax.numpy as jnp
import numpy as np
from jax import lax
from jax.experimental import pallas as pl
from jax.experimental.pallas import tpu as pltpu
from jax.sharding import PartitionSpec as P

highest = lax.Precision.HIGHEST
f32 = jnp.float32
bf16 = jnp.bfloat16
LANES = 128
STEP = 32


def tables(length):
    freq = np.arange(length)
    hi = (np.arange(length // STEP)[:, None] * STEP * freq) % (2 * length)
    lo = (np.arange(STEP)[:, None] * freq) % (2 * length)
    scale = math.pi / length
    pack = lambda p: np.stack([np.cos(p * scale), np.sin(p * scale)]).astype(np.float32)
    return pack(hi), pack(lo)


def product_kernel(go_ref, po_ref, pr_ref, vb_ref, out_ref):
    out_ref[0, 0] = (go_ref[0].astype(f32) * po_ref[0].astype(f32)).astype(bf16)
    out_ref[0, 1] = (pr_ref[0].astype(f32) * vb_ref[0].astype(f32)).astype(bf16)


def product(grad_output, post_gate, pre_gate, value_branch, groups):
    _, channels, block = grad_output.shape
    rows = channels // groups
    spec = pl.BlockSpec((1, rows, block), lambda i: (0, i, 0))
    return pl.pallas_call(
        product_kernel,
        grid=(groups,),
        in_specs=[spec] * 4,
        out_specs=pl.BlockSpec((1, 2, rows, block), lambda i: (i, 0, 0, 0)),
        out_shape=jax.ShapeDtypeStruct((groups, 2, rows, block), bf16),
        cost_estimate=pl.CostEstimate(
            flops=2 * channels * block, bytes_accessed=12 * channels * block, transcendentals=0
        ),
        name="product",
    )(grad_output, post_gate, pre_gate, value_branch)


def filter_kernel(filt_ref, hi_ref, lo_ref, w_ref, spec_ref):
    n = pl.program_id(0)
    length = filt_ref.shape[1]
    lo_cos = lo_ref[0]
    lo_sin = lo_ref[1]
    lane = lax.broadcasted_iota(jnp.int32, (STEP, LANES), 1)
    row = lax.broadcasted_iota(jnp.int32, (STEP, LANES), 0)
    first = jnp.logical_and(lane == 0, n == 0)
    nyquist = jnp.where(row % 2 == 0, 1.0, -1.0).astype(f32)
    for i in range(length // STEP):
        hi_cos = hi_ref[0, i : i + 1, :]
        hi_sin = hi_ref[1, i : i + 1, :]
        cosine = hi_cos * lo_cos - hi_sin * lo_sin
        sine = hi_sin * lo_cos + hi_cos * lo_sin
        rows = pl.ds(i * STEP, STEP)
        w_ref[rows, :LANES] = cosine.astype(bf16)
        w_ref[rows, LANES:] = jnp.where(first, nyquist, -sine).astype(bf16)
    spec_ref[...] = jnp.dot(
        filt_ref[...].astype(bf16), w_ref[...], preferred_element_type=f32
    )


def filter_spectrum_dense(filt):
    channels, length = filt.shape
    hi, lo = tables(length)
    tiles = length // LANES
    return pl.pallas_call(
        filter_kernel,
        grid=(tiles,),
        in_specs=[
            pl.BlockSpec((channels, length), lambda n: (0, 0)),
            pl.BlockSpec((2, length // STEP, LANES), lambda n: (0, 0, n)),
            pl.BlockSpec((2, STEP, LANES), lambda n: (0, 0, n)),
        ],
        out_specs=[
            pl.BlockSpec((length, 2 * LANES), lambda n: (0, n)),
            pl.BlockSpec((channels, 2 * LANES), lambda n: (0, n)),
        ],
        out_shape=[
            jax.ShapeDtypeStruct((length, 2 * length), bf16),
            jax.ShapeDtypeStruct((channels, 2 * length), f32),
        ],
        compiler_params=pltpu.CompilerParams(vmem_limit_bytes=16 * 2**20),
        cost_estimate=pl.CostEstimate(
            flops=4 * channels * length * length,
            bytes_accessed=4 * channels * length * 3 + 4 * length * length,
            transcendentals=0,
        ),
        name="filter_spectrum",
    )(filt, jnp.asarray(hi), jnp.asarray(lo))


def correlate_kernel(got_ref, w_ref, spec_ref, corr_ref, grad_ref, rows_ref, prod_ref):
    groups, _, channels, block = got_ref.shape
    length = groups * block
    for p in range(groups):
        cols = pl.ds(p * block, block)
        rows_ref[:channels, cols] = got_ref[p, 0]
        rows_ref[channels:, cols] = got_ref[p, 1]
    lane = lax.broadcasted_iota(jnp.int32, (channels, LANES), 1)
    for n in range(length // LANES):
        re = pl.ds(2 * n * LANES, LANES)
        im = pl.ds((2 * n + 1) * LANES, LANES)
        both = pl.ds(2 * n * LANES, 2 * LANES)
        spectrum = jnp.dot(rows_ref[...], w_ref[:, both], preferred_element_type=f32)
        g_re = spectrum[:channels, :LANES]
        g_im = spectrum[:channels, LANES:]
        s_re = spectrum[channels:, :LANES]
        s_im = spectrum[channels:, LANES:]
        h_re = spec_ref[:, re]
        h_im = spec_ref[:, im]
        for y_re, y_im, at in ((h_re, h_im, 0), (s_re, s_im, channels)):
            rr = g_re * y_re
            ii = g_im * y_im
            cross = g_im * y_re - g_re * y_im
            scale = 1.0 / length
            if n == 0:
                first = lane == 0
                real = jnp.where(first, rr, rr + ii)
                imag = jnp.where(first, ii, cross)
                scale = jnp.where(first, 0.5 / length, 1.0 / length)
            else:
                real = rr + ii
                imag = cross
            out = pl.ds(at, channels)
            prod_ref[out, re] = (real * scale).astype(bf16)
            prod_ref[out, im] = (imag * scale).astype(bf16)
    taps = grad_ref.shape[2]
    tile = 2 * LANES
    for q in range(length // tile):
        out = lax.dot_general(
            prod_ref[...],
            w_ref[pl.ds(q * tile, tile), :],
            (((1,), (1,)), ((), ())),
            preferred_element_type=f32,
        )
        for part in range(tile // block):
            corr_ref[q * (tile // block) + part] = out[
                :channels, part * block : (part + 1) * block
            ].astype(bf16)
        start = q * tile
        grad_ref[start // taps, :, pl.ds(start % taps, tile)] = out[channels:].astype(bf16)


def correlate_dense(got, w, spec, shares):
    groups, _, channels, block = got.shape
    length = groups * block
    vmem = pl.BlockSpec(memory_space=pltpu.VMEM)
    return pl.pallas_call(
        correlate_kernel,
        in_specs=[vmem] * 3,
        out_specs=[vmem] * 2,
        out_shape=[
            jax.ShapeDtypeStruct((groups, channels, block), bf16),
            jax.ShapeDtypeStruct((shares, channels, length // shares), bf16),
        ],
        scratch_shapes=[
            pltpu.VMEM((2 * channels, length), bf16),
            pltpu.VMEM((2 * channels, 2 * length), bf16),
        ],
        compiler_params=pltpu.CompilerParams(vmem_limit_bytes=32 * 2**20),
        cost_estimate=pl.CostEstimate(
            flops=16 * channels * length * length,
            bytes_accessed=4 * length * length + 20 * channels * length,
            transcendentals=0,
        ),
        name="correlate",
    )(got, w, spec)


def shards_dense(grad_output, post_gate, pre_gate, value_branch, long_filter, skip_weight):
    groups = lax.axis_size("ctx")
    shares = lax.axis_size("dp")
    seqs, channels, block = grad_output.shape
    length = long_filter.shape[1]
    token_count = seqs * shares * length
    sent = product(grad_output, post_gate, pre_gate, value_branch, groups)
    w, spec = filter_spectrum_dense(long_filter)
    got = lax.all_to_all(sent, "ctx", split_axis=0, concat_axis=0, tiled=True)
    corr, grad = correlate_dense(got, w, spec, shares)
    back = lax.all_to_all(corr, "ctx", split_axis=0, concat_axis=0, tiled=True)
    terms = lax.all_to_all(grad, "dp", split_axis=0, concat_axis=0, tiled=True)
    returned = back.reshape(seqs, channels, block)
    gated = (grad_output.astype(f32) * post_gate.astype(f32)).astype(bf16)
    summed = returned.astype(f32) + skip_weight[None, :, None] * gated.astype(f32)
    grad_pre_gate = (summed * value_branch.astype(f32)).astype(bf16)
    grad_value_branch = (summed * pre_gate.astype(f32)).astype(bf16)
    grad_long_filter = jnp.sum(terms.astype(f32), axis=0) * (1.0 / math.sqrt(token_count))
    return (grad_pre_gate, grad_value_branch, grad_long_filter)


def split_factor(length):
    for candidate in range(128, 1, -1):
        if length % candidate == 0:
            return candidate
    return 1


def twiddle(row_count, col_count, modulus, sign_value):
    row_index = lax.broadcasted_iota(jnp.int32, (row_count, col_count), 0)
    col_index = lax.broadcasted_iota(jnp.int32, (row_count, col_count), 1)
    phases = row_index * col_index % modulus
    angles = phases.astype(jnp.float32) * (2.0 * math.pi / modulus)
    return (jnp.cos(angles), sign_value * jnp.sin(angles))


def block_matrix(row_count, col_count, modulus, sign_value, part_count):
    cosine, sine = twiddle(row_count, col_count, modulus, sign_value)
    matrix = jnp.stack([jnp.stack([cosine, sine], 1), jnp.stack([-sine, cosine], 1)], 0)
    return matrix[:part_count]


def transform(parts, sign_value, length):
    part_count = parts.shape[0]
    width = parts.shape[-1]
    leading = split_factor(length)
    if length <= 256 or leading == 1 or leading == length:
        matrix = block_matrix(width, length, length, sign_value, part_count)
        return jnp.einsum("p...j,pjqk->q...k", parts, matrix, precision=highest)
    trailing = length // leading
    live = -(-width // trailing)
    if live * trailing != width:
        extra = [(0, 0)] * (parts.ndim - 1) + [(0, live * trailing - width)]
        parts = jnp.pad(parts, extra)
    batch_dims = parts.shape[1:-1]
    parts = parts.reshape((part_count,) + batch_dims + (live, trailing))
    matrix = block_matrix(live, leading, leading, sign_value, part_count)
    first = jnp.einsum("p...jb,pjqk->q...kb", parts, matrix, precision=highest)
    turn_cos, turn_sin = twiddle(leading, trailing, length, sign_value)
    rotated = jnp.stack(
        [first[0] * turn_cos - first[1] * turn_sin, first[0] * turn_sin + first[1] * turn_cos], 0
    )
    deep = transform(rotated, sign_value, trailing)
    return jnp.swapaxes(deep, -1, -2).reshape((2,) + batch_dims + (length,))


def mirror(values):
    return jnp.roll(jnp.flip(values, -1), 1, -1)


def filter_spectrum(filter_rows):
    length = filter_rows.shape[1]
    spectrum = transform(filter_rows[None], -1.0, 2 * length)
    return (spectrum[0], spectrum[1])


def correlate(grad_rows, saved_rows, filt_real, filt_imag):
    length = grad_rows.shape[2]
    padded = 2 * length
    stacked = jnp.stack([grad_rows.astype(jnp.float32), saved_rows.astype(jnp.float32)], 0)
    spectrum = transform(stacked, -1.0, padded)
    spec_real = spectrum[0]
    spec_imag = spectrum[1]
    flip_real = mirror(spec_real)
    flip_imag = mirror(spec_imag)
    grad_real = 0.5 * (spec_real + flip_real)
    grad_imag = 0.5 * (spec_imag - flip_imag)
    input_real = 0.5 * (spec_imag + flip_imag)
    input_imag = 0.5 * (flip_real - spec_real)
    first_real = filt_real * grad_real + filt_imag * grad_imag
    first_imag = filt_real * grad_imag - filt_imag * grad_real
    second_real = grad_real * input_real + grad_imag * input_imag
    second_imag = grad_imag * input_real - grad_real * input_imag
    combined = jnp.stack([first_real - second_imag, first_imag + second_real], 0)
    result = transform(combined, 1.0, padded)
    factor = 1.0 / padded
    correlated = (result[0, ..., :length] * factor).astype(jnp.bfloat16)
    filter_terms = result[1, ..., :length] * factor
    return (correlated, filter_terms)


def shards_long(grad_output, post_gate, pre_gate, value_branch, long_filter, skip_weight):
    seq_count = grad_output.shape[0]
    length = long_filter.shape[1]
    token_count = seq_count * lax.axis_size("dp") * length
    gated = (grad_output.astype(jnp.float32) * post_gate.astype(jnp.float32)).astype(jnp.bfloat16)
    saved = (pre_gate.astype(jnp.float32) * value_branch.astype(jnp.float32)).astype(jnp.bfloat16)
    filt_real, filt_imag = filter_spectrum(long_filter)
    correlated, filter_terms = correlate(
        lax.all_to_all(gated, "ctx", split_axis=1, concat_axis=2, tiled=True),
        lax.all_to_all(saved, "ctx", split_axis=1, concat_axis=2, tiled=True),
        filt_real,
        filt_imag,
    )
    back = lax.all_to_all(correlated, "ctx", split_axis=2, concat_axis=1, tiled=True)
    returned, filter_terms = (back, filter_terms)
    filter_sum = jnp.sum(filter_terms, axis=0)
    shares = lax.psum_scatter(
        filter_sum.astype(jnp.bfloat16), "dp", scatter_dimension=1, tiled=True
    ).astype(jnp.float32)
    summed = returned.astype(jnp.float32) + skip_weight[None, :, None] * gated.astype(jnp.float32)
    grad_pre_gate = (summed * value_branch.astype(jnp.float32)).astype(jnp.bfloat16)
    grad_value_branch = (summed * pre_gate.astype(jnp.float32)).astype(jnp.bfloat16)
    grad_long_filter = shares * (1.0 / math.sqrt(token_count))
    return (grad_pre_gate, grad_value_branch, grad_long_filter)


def shards(grad_output, post_gate, pre_gate, value_branch, long_filter, skip_weight):
    seqs, _, block = grad_output.shape
    rows, length = long_filter.shape
    shares = lax.axis_size("dp")
    dense = (
        seqs == 1
        and length <= 1024
        and block == LANES
        and rows % 16 == 0
        and length % (2 * LANES * shares) == 0
    )
    body = shards_dense if dense else shards_long
    return body(grad_output, post_gate, pre_gate, value_branch, long_filter, skip_weight)


def solution(mesh):
    return jax.shard_map(
        shards,
        mesh=mesh,
        in_specs=(
            P("dp", None, "ctx"),
            P("dp", None, "ctx"),
            P("dp", None, "ctx"),
            P("dp", None, "ctx"),
            P("ctx", None),
            P(),
        ),
        out_specs=(P("dp", None, "ctx"), P("dp", None, "ctx"), P("ctx", "dp")),
        check_vma=False,
    )
```

```python
import functools
import math

import jax
import jax.numpy as jnp
import numpy as np
from jax import lax
from jax.experimental import pallas as pl
from jax.experimental.pallas import tpu as pltpu
from jax.sharding import PartitionSpec as P


highest = lax.Precision.HIGHEST
f32 = jnp.float32
bf16 = jnp.bfloat16
LANES = 128
STEP = 32
VMEM_LIMIT = 16 * 2**20


def tables(length):
    freq = np.arange(length)
    hi = (np.arange(length // STEP)[:, None] * STEP * freq) % (2 * length)
    lo = (np.arange(STEP)[:, None] * freq) % (2 * length)
    scale = math.pi / length
    pack = lambda p: np.stack([np.cos(p * scale), np.sin(p * scale)]).astype(np.float32)
    return pack(hi), pack(lo)


def in_hbm(*arrays):
    return [pltpu.with_memory_space_constraint(array, pltpu.HBM) for array in arrays]


def row_block(axis, offset, count, rows):
    return pl.ds(pl.multiple_of(lax.rem(lax.axis_index(axis) + offset, count) * rows, rows), rows)


def product_kernel(axis, *refs):
    count = len(refs) - 6
    in_refs, out_refs = refs[:4], refs[4 : 4 + count]
    buf_ref, sems = refs[4 + count :]
    rows = out_refs[0].shape[1]
    copies = []
    for k in range(count):
        block = row_block(axis, k, count, rows)
        copies.append(
            [
                pltpu.make_async_copy(in_ref.at[block], buf_ref.at[j, k], sems.at[j, k])
                for j, in_ref in enumerate(in_refs)
            ]
        )
        for copy in copies[k]:
            copy.start()
    for k, out_ref in enumerate(out_refs):
        for copy in copies[k]:
            copy.wait()
        for j in range(2):
            left = buf_ref[2 * j, k].astype(f32)
            out_ref[j] = (left * buf_ref[2 * j + 1, k].astype(f32)).astype(bf16)


def product(grad_output, post_gate, pre_gate, value_branch, axis):
    count = lax.axis_size(axis)
    channels, block = grad_output.shape
    rows = channels // count
    return pl.pallas_call(
        functools.partial(product_kernel, axis),
        in_specs=[pl.BlockSpec(memory_space=pltpu.HBM)] * 4,
        out_specs=[pl.BlockSpec(memory_space=pltpu.VMEM)] * count,
        out_shape=[jax.ShapeDtypeStruct((2, rows, block), bf16)] * count,
        scratch_shapes=[
            pltpu.VMEM((4, count, rows, block), bf16),
            pltpu.SemaphoreType.DMA((4, count)),
        ],
        compiler_params=pltpu.CompilerParams(vmem_limit_bytes=4 * 2**20),
        cost_estimate=pl.CostEstimate(
            flops=2 * channels * block, bytes_accessed=12 * channels * block, transcendentals=0
        ),
        name="product",
    )(*in_hbm(grad_output, post_gate, pre_gate, value_branch))


def filter_kernel(filt_ref, hi_ref, lo_ref, w_ref, spec_ref):
    n = pl.program_id(0)
    length = filt_ref.shape[1]
    lo_cos = lo_ref[0]
    lo_sin = lo_ref[1]
    lane = lax.broadcasted_iota(jnp.int32, (STEP, LANES), 1)
    row = lax.broadcasted_iota(jnp.int32, (STEP, LANES), 0)
    first = jnp.logical_and(lane == 0, n == 0)
    nyquist = jnp.where(row % 2 == 0, 1.0, -1.0).astype(f32)
    for i in range(length // STEP):
        hi_cos = hi_ref[0, i : i + 1, :]
        hi_sin = hi_ref[1, i : i + 1, :]
        cosine = hi_cos * lo_cos - hi_sin * lo_sin
        sine = hi_sin * lo_cos + hi_cos * lo_sin
        rows = pl.ds(i * STEP, STEP)
        w_ref[rows, :LANES] = cosine.astype(bf16)
        w_ref[rows, LANES:] = jnp.where(first, nyquist, -sine).astype(bf16)
    spec_ref[...] = jnp.dot(
        filt_ref[...].astype(bf16), w_ref[...], preferred_element_type=f32
    )


def filter_spectrum_dense(filt):
    channels, length = filt.shape
    hi, lo = tables(length)
    tiles = length // LANES
    return pl.pallas_call(
        filter_kernel,
        grid=(tiles,),
        in_specs=[
            pl.BlockSpec((channels, length), lambda n: (0, 0)),
            pl.BlockSpec((2, length // STEP, LANES), lambda n: (0, 0, n)),
            pl.BlockSpec((2, STEP, LANES), lambda n: (0, 0, n)),
        ],
        out_specs=[
            pl.BlockSpec((length, 2 * LANES), lambda n: (0, n)),
            pl.BlockSpec((channels, 2 * LANES), lambda n: (0, n)),
        ],
        out_shape=[
            jax.ShapeDtypeStruct((length, 2 * length), bf16),
            jax.ShapeDtypeStruct((channels, 2 * length), f32),
        ],
        compiler_params=pltpu.CompilerParams(vmem_limit_bytes=16 * 2**20),
        cost_estimate=pl.CostEstimate(
            flops=4 * channels * length * length,
            bytes_accessed=4 * channels * length * 3 + 4 * length * length,
            transcendentals=0,
        ),
        name="filter_spectrum",
    )(*in_hbm(filt, jnp.asarray(hi), jnp.asarray(lo)))


def multiply_spectra(a_re, a_im, b_re, b_im, first_tile, length):
    rr = a_re * b_re
    ii = a_im * b_im
    cross = a_im * b_re - a_re * b_im
    if not first_tile:
        return (rr + ii) * (1.0 / length), cross * (1.0 / length)
    first = lax.broadcasted_iota(jnp.int32, rr.shape, 1) == 0
    scale = jnp.where(first, 0.5 / length, 1.0 / length)
    return jnp.where(first, rr, rr + ii) * scale, jnp.where(first, ii, cross) * scale


def inverse(prod_ref, w_ref, taps):
    return lax.dot_general(
        prod_ref[...], w_ref[taps, :], (((1,), (1,)), ((), ())), preferred_element_type=f32
    ).astype(bf16)


def correlate_kernel(axis, w_ref, spec_ref, *refs):
    count = (len(refs) - 3) // 2
    got_refs, out_refs = refs[:count], refs[count : 2 * count]
    terms_ref, rows_ref, prod_ref = refs[2 * count :]
    _, channels, block = got_refs[0].shape
    length = count * block
    me = lax.axis_index(axis)
    for k, got_ref in enumerate(got_refs):
        rows_ref[lax.rem(me + count - k, count)] = got_ref[...]
    rows = jnp.concatenate(
        [rows_ref[p].reshape(2 * channels, block) for p in range(count)], axis=1
    )
    for n in range(length // LANES):
        re = pl.ds(2 * n * LANES, LANES)
        im = pl.ds((2 * n + 1) * LANES, LANES)
        both = pl.ds(2 * n * LANES, 2 * LANES)
        spectrum = jnp.dot(rows, w_ref[:, both], preferred_element_type=f32)
        g_re = spectrum[:channels, :LANES]
        g_im = spectrum[:channels, LANES:]
        for y_re, y_im, out_ref in (
            (spec_ref[:, re], spec_ref[:, im], prod_ref),
            (spectrum[channels:, :LANES], spectrum[channels:, LANES:], terms_ref),
        ):
            real, imag = multiply_spectra(g_re, g_im, y_re, y_im, n == 0, length)
            out_ref[:, re] = real.astype(bf16)
            out_ref[:, im] = imag.astype(bf16)
    pair = 2 * LANES // block
    for q in range(count // pair):
        out = inverse(prod_ref, w_ref, pl.ds(q * 2 * LANES, 2 * LANES))
        for part in range(pair):
            rows_ref[q * pair + part, 0] = out[:, part * block : (part + 1) * block]
    for k, out_ref in enumerate(out_refs):
        out_ref[...] = rows_ref[lax.rem(me + k, count), 0]


def correlate_dense(got, w, spec, axis):
    count = len(got)
    _, channels, block = got[0].shape
    length = count * block
    vmem = pl.BlockSpec(memory_space=pltpu.VMEM)
    *corr, terms = pl.pallas_call(
        functools.partial(correlate_kernel, axis),
        in_specs=[vmem] * (2 + count),
        out_specs=[vmem] * (count + 1),
        out_shape=[jax.ShapeDtypeStruct((channels, block), bf16)] * count
        + [jax.ShapeDtypeStruct((channels, 2 * length), bf16)],
        scratch_shapes=[
            pltpu.VMEM((count, 2, channels, block), bf16),
            pltpu.VMEM((channels, 2 * length), bf16),
        ],
        compiler_params=pltpu.CompilerParams(vmem_limit_bytes=VMEM_LIMIT),
        cost_estimate=pl.CostEstimate(
            flops=12 * channels * length * length,
            bytes_accessed=4 * length * length + 20 * channels * length,
            transcendentals=0,
        ),
        name="correlate",
    )(w, spec, *got)
    return corr, terms


def gradient_kernel(axis, w_ref, terms_ref, *out_refs):
    shares = len(out_refs)
    taps = out_refs[0].shape[1]
    for k, out_ref in enumerate(out_refs):
        out_ref[...] = inverse(terms_ref, w_ref, row_block(axis, k, shares, taps))


def gradient_dense(terms, w, axis):
    shares = lax.axis_size(axis)
    channels = terms.shape[0]
    length = terms.shape[1] // 2
    vmem = pl.BlockSpec(memory_space=pltpu.VMEM)
    return pl.pallas_call(
        functools.partial(gradient_kernel, axis),
        in_specs=[vmem] * 2,
        out_specs=[vmem] * shares,
        out_shape=[jax.ShapeDtypeStruct((channels, length // shares), bf16)] * shares,
        compiler_params=pltpu.CompilerParams(vmem_limit_bytes=VMEM_LIMIT),
        cost_estimate=pl.CostEstimate(
            flops=4 * channels * length * length,
            bytes_accessed=4 * length * length + 6 * channels * length,
            transcendentals=0,
        ),
        name="gradient",
    )(w, terms)


def finish_kernel(axis, shares, scale, base_ref, pr_ref, vb_ref, *refs):
    count = len(refs) - shares - 7
    back_refs, term_refs = refs[:count], refs[count : count + shares]
    pre_out, value_out, grad_out, pre_buf, value_buf, grad_buf, sems = refs[count + shares :]
    rows = back_refs[0].shape[0]
    copies = []

    def send(source, target, sem):
        copy = pltpu.make_async_copy(source, target, sem)
        copy.start()
        copies.append(copy)

    for k, back_ref in enumerate(back_refs):
        block = row_block(axis, count - k, count, rows)
        summed = back_ref[...].astype(f32) + base_ref[block]
        pre_buf[k] = (summed * vb_ref[block].astype(f32)).astype(bf16)
        value_buf[k] = (summed * pr_ref[block].astype(f32)).astype(bf16)
        send(pre_buf.at[k], pre_out.at[block], sems.at[0, k])
        send(value_buf.at[k], value_out.at[block], sems.at[1, k])
    grad_buf[...] = sum(term_ref[...].astype(f32) for term_ref in term_refs) * scale
    send(grad_buf, grad_out, sems.at[2, 0])
    for copy in copies:
        copy.wait()


def finish(back, base, pre_gate, value_branch, terms, scale, axis):
    count = len(back)
    shares = len(terms)
    rows, block = back[0].shape
    channels = count * rows
    vmem = pl.BlockSpec(memory_space=pltpu.VMEM)
    return pl.pallas_call(
        functools.partial(finish_kernel, axis, shares, scale),
        in_specs=[vmem] * (3 + count + shares),
        out_specs=[pl.BlockSpec(memory_space=pltpu.HBM)] * 3,
        out_shape=[jax.ShapeDtypeStruct((channels, block), bf16)] * 2
        + [jax.ShapeDtypeStruct(terms[0].shape, f32)],
        scratch_shapes=[
            pltpu.VMEM((count, rows, block), bf16),
            pltpu.VMEM((count, rows, block), bf16),
            pltpu.VMEM(terms[0].shape, f32),
            pltpu.SemaphoreType.DMA((3, count)),
        ],
        compiler_params=pltpu.CompilerParams(vmem_limit_bytes=8 * 2**20),
        cost_estimate=pl.CostEstimate(
            flops=3 * channels * block, bytes_accessed=14 * channels * block, transcendentals=0
        ),
        name="finish",
    )(base, pre_gate, value_branch, *back, *terms)


def ahead(value, axis, k):
    count = lax.axis_size(axis)
    return lax.ppermute(value, axis, [(j, (j + k) % count) for j in range(count)])


def exchange(blocks, axis):
    got = [blocks[0]]
    for k in range(1, len(blocks)):
        got.append(ahead(blocks[k], axis, k))
    return got


def shards_dense(grad_output, post_gate, pre_gate, value_branch, long_filter, skip_weight):
    shares = lax.axis_size("dp")
    seqs, channels, block = grad_output.shape
    length = long_filter.shape[1]
    token_count = seqs * shares * length
    grad_rows, post_rows, pre_rows, value_rows = (
        x.reshape(channels, block) for x in (grad_output, post_gate, pre_gate, value_branch)
    )
    sent = product(grad_rows, post_rows, pre_rows, value_rows, "ctx")
    got = exchange(sent, "ctx")
    w, spec = filter_spectrum_dense(long_filter)
    gated = (grad_rows.astype(f32) * post_rows.astype(f32)).astype(bf16)
    base = skip_weight[:, None] * gated.astype(f32)
    corr, terms = correlate_dense(got, w, spec, "ctx")
    back = exchange(corr, "ctx")
    terms = gradient_dense(terms, w, "dp")
    terms = exchange(terms, "dp")
    grad_pre_gate, grad_value_branch, grad_long_filter = finish(
        back, base, pre_rows, value_rows, terms, 1.0 / math.sqrt(token_count), "ctx"
    )
    shape = grad_output.shape
    return (grad_pre_gate.reshape(shape), grad_value_branch.reshape(shape), grad_long_filter)


def split_factor(length):
    for candidate in range(128, 1, -1):
        if length % candidate == 0:
            return candidate
    return 1


def twiddle(row_count, col_count, modulus, sign_value):
    row_index = lax.broadcasted_iota(jnp.int32, (row_count, col_count), 0)
    col_index = lax.broadcasted_iota(jnp.int32, (row_count, col_count), 1)
    phases = row_index * col_index % modulus
    angles = phases.astype(jnp.float32) * (2.0 * math.pi / modulus)
    return (jnp.cos(angles), sign_value * jnp.sin(angles))


def block_matrix(row_count, col_count, modulus, sign_value, part_count):
    cosine, sine = twiddle(row_count, col_count, modulus, sign_value)
    matrix = jnp.stack([jnp.stack([cosine, sine], 1), jnp.stack([-sine, cosine], 1)], 0)
    return matrix[:part_count]


def transform(parts, sign_value, length):
    part_count = parts.shape[0]
    width = parts.shape[-1]
    leading = split_factor(length)
    if length <= 256 or leading == 1 or leading == length:
        matrix = block_matrix(width, length, length, sign_value, part_count)
        return jnp.einsum("p...j,pjqk->q...k", parts, matrix, precision=highest)
    trailing = length // leading
    live = -(-width // trailing)
    if live * trailing != width:
        extra = [(0, 0)] * (parts.ndim - 1) + [(0, live * trailing - width)]
        parts = jnp.pad(parts, extra)
    batch_dims = parts.shape[1:-1]
    parts = parts.reshape((part_count,) + batch_dims + (live, trailing))
    matrix = block_matrix(live, leading, leading, sign_value, part_count)
    first = jnp.einsum("p...jb,pjqk->q...kb", parts, matrix, precision=highest)
    turn_cos, turn_sin = twiddle(leading, trailing, length, sign_value)
    rotated = jnp.stack(
        [first[0] * turn_cos - first[1] * turn_sin, first[0] * turn_sin + first[1] * turn_cos], 0
    )
    deep = transform(rotated, sign_value, trailing)
    return jnp.swapaxes(deep, -1, -2).reshape((2,) + batch_dims + (length,))


def mirror(values):
    return jnp.roll(jnp.flip(values, -1), 1, -1)


def filter_spectrum(filter_rows):
    length = filter_rows.shape[1]
    spectrum = transform(filter_rows[None], -1.0, 2 * length)
    return (spectrum[0], spectrum[1])


def correlate(grad_rows, saved_rows, filt_real, filt_imag):
    length = grad_rows.shape[2]
    padded = 2 * length
    stacked = jnp.stack([grad_rows.astype(jnp.float32), saved_rows.astype(jnp.float32)], 0)
    spectrum = transform(stacked, -1.0, padded)
    spec_real = spectrum[0]
    spec_imag = spectrum[1]
    flip_real = mirror(spec_real)
    flip_imag = mirror(spec_imag)
    grad_real = 0.5 * (spec_real + flip_real)
    grad_imag = 0.5 * (spec_imag - flip_imag)
    input_real = 0.5 * (spec_imag + flip_imag)
    input_imag = 0.5 * (flip_real - spec_real)
    first_real = filt_real * grad_real + filt_imag * grad_imag
    first_imag = filt_real * grad_imag - filt_imag * grad_real
    second_real = grad_real * input_real + grad_imag * input_imag
    second_imag = grad_imag * input_real - grad_real * input_imag
    combined = jnp.stack([first_real - second_imag, first_imag + second_real], 0)
    result = transform(combined, 1.0, padded)
    factor = 1.0 / padded
    correlated = (result[0, ..., :length] * factor).astype(jnp.bfloat16)
    filter_terms = result[1, ..., :length] * factor
    return (correlated, filter_terms)


def shards_long(grad_output, post_gate, pre_gate, value_branch, long_filter, skip_weight):
    seq_count = grad_output.shape[0]
    length = long_filter.shape[1]
    token_count = seq_count * lax.axis_size("dp") * length
    gated = (grad_output.astype(jnp.float32) * post_gate.astype(jnp.float32)).astype(jnp.bfloat16)
    saved = (pre_gate.astype(jnp.float32) * value_branch.astype(jnp.float32)).astype(jnp.bfloat16)
    filt_real, filt_imag = filter_spectrum(long_filter)
    correlated, filter_terms = correlate(
        lax.all_to_all(gated, "ctx", split_axis=1, concat_axis=2, tiled=True),
        lax.all_to_all(saved, "ctx", split_axis=1, concat_axis=2, tiled=True),
        filt_real,
        filt_imag,
    )
    back = lax.all_to_all(correlated, "ctx", split_axis=2, concat_axis=1, tiled=True)
    returned, filter_terms = (back, filter_terms)
    filter_sum = jnp.sum(filter_terms, axis=0)
    shares = lax.psum_scatter(
        filter_sum.astype(jnp.bfloat16), "dp", scatter_dimension=1, tiled=True
    ).astype(jnp.float32)
    summed = returned.astype(jnp.float32) + skip_weight[None, :, None] * gated.astype(jnp.float32)
    grad_pre_gate = (summed * value_branch.astype(jnp.float32)).astype(jnp.bfloat16)
    grad_value_branch = (summed * pre_gate.astype(jnp.float32)).astype(jnp.bfloat16)
    grad_long_filter = shares * (1.0 / math.sqrt(token_count))
    return (grad_pre_gate, grad_value_branch, grad_long_filter)


def shards(grad_output, post_gate, pre_gate, value_branch, long_filter, skip_weight):
    seqs, _, block = grad_output.shape
    rows, length = long_filter.shape
    shares = lax.axis_size("dp")
    dense = (
        seqs == 1
        and length <= 1024
        and block == LANES
        and rows % 16 == 0
        and length % (2 * LANES * shares) == 0
    )
    body = shards_dense if dense else shards_long
    return body(grad_output, post_gate, pre_gate, value_branch, long_filter, skip_weight)


def solution(mesh):
    return jax.shard_map(
        shards,
        mesh=mesh,
        in_specs=(
            P("dp", None, "ctx"),
            P("dp", None, "ctx"),
            P("dp", None, "ctx"),
            P("dp", None, "ctx"),
            P("ctx", None),
            P(),
        ),
        out_specs=(P("dp", None, "ctx"), P("dp", None, "ctx"), P("ctx", "dp")),
        check_vma=False,
    )
```

```python
import functools
import math

import jax
import jax.numpy as jnp
import numpy as np
from jax import lax
from jax.experimental import pallas as pl
from jax.experimental.pallas import tpu as pltpu
from jax.sharding import PartitionSpec as P


highest = lax.Precision.HIGHEST
f32 = jnp.float32
bf16 = jnp.bfloat16
LANES = 128
VMEM_MIB = 12


def half_matrix(length):
    time = np.arange(length // 2)[:, None]
    phase = (time * np.arange(length)[None, :] % (2 * length)) * (math.pi / length)
    pair = np.stack([np.cos(phase), -np.sin(phase)], axis=1)
    pair[:, 1, 0] = 1.0 - 2.0 * (time[:, 0] % 2)
    tiles = pair.reshape(length // 2, 2, length // LANES, LANES).transpose(0, 2, 1, 3)
    return jnp.asarray(tiles.reshape(length // 2, 2 * length), bf16)


def in_hbm(*arrays):
    return [pltpu.with_memory_space_constraint(array, pltpu.HBM) for array in arrays]


def peer_rows(axis, k, rows):
    return pl.ds(pl.multiple_of((lax.axis_index(axis) ^ k) * rows, rows), rows)


def call(kernel, out_specs, out_shape, scratch, flops, moved, mib, operands, in_specs=None):
    vmem = pl.BlockSpec(memory_space=pltpu.VMEM)
    return list(pl.pallas_call(
        kernel,
        in_specs=in_specs or [vmem] * len(operands),
        out_specs=out_specs or [vmem] * len(out_shape),
        out_shape=out_shape,
        scratch_shapes=scratch,
        compiler_params=pltpu.CompilerParams(vmem_limit_bytes=mib * 2**20),
        cost_estimate=pl.CostEstimate(flops=flops, bytes_accessed=moved, transcendentals=0),
    )(*operands))


def product_kernel(axis, near, far, *refs):
    in_refs, out_refs = refs[:4], refs[4:-2]
    buf_ref, sems = refs[-2:]
    both_refs = dict(zip(near, out_refs))
    gated_refs = dict(zip(far, out_refs[len(near) :]))
    saved_refs = dict(zip(far, out_refs[len(near) + len(far) :]))
    rows = buf_ref.shape[2]
    copies = {}
    for k in far + near:
        copies[k] = [
            pltpu.make_async_copy(
                in_ref.at[peer_rows(axis, k, rows)], buf_ref.at[j, k], sems.at[j, k]
            )
            for j, in_ref in enumerate(in_refs)
        ]
        for copy in copies[k]:
            copy.start()
    for k in far + near:
        for copy in copies[k]:
            copy.wait()
        gated = (buf_ref[0, k].astype(f32) * buf_ref[1, k].astype(f32)).astype(bf16)
        saved = (buf_ref[2, k].astype(f32) * buf_ref[3, k].astype(f32)).astype(bf16)
        if k in both_refs:
            both_refs[k][0] = gated
            both_refs[k][1] = saved
        else:
            gated_refs[k][...] = gated
            saved_refs[k][...] = saved


def product(arrays, near, far, axis):
    count = len(near) + len(far)
    channels, block = arrays[0].shape
    rows = channels // count
    out = call(
        functools.partial(product_kernel, axis, near, far),
        None,
        [jax.ShapeDtypeStruct((2, rows, block), bf16)] * len(near)
        + [jax.ShapeDtypeStruct((rows, block), bf16)] * (2 * len(far)),
        [pltpu.VMEM((4, count, rows, block), bf16), pltpu.SemaphoreType.DMA((4, count))],
        2 * channels * block,
        12 * channels * block,
        4,
        in_hbm(*arrays),
        [pl.BlockSpec(memory_space=pltpu.HBM)] * 4,
    )
    ends = [len(near), count, count + len(far)]
    return [dict(zip(ks, out[lo:hi])) for ks, lo, hi in zip((near, far, far), [0] + ends, ends)]


def filter_kernel(filt_ref, low_ref, high_ref, spec_ref):
    length = filt_ref.shape[1]
    half = length // 2
    filt = filt_ref[...].astype(bf16)
    turn = lax.broadcasted_iota(jnp.int32, (1, LANES), 1) % 4
    keep = jnp.where(turn == 0, 1.0, jnp.where(turn == 2, -1.0, 0.0)).astype(bf16)
    swap = jnp.where(turn == 1, 1.0, jnp.where(turn == 3, -1.0, 0.0)).astype(bf16)
    for n in range(length // LANES):
        re = pl.ds(2 * n * LANES, LANES)
        im = pl.ds((2 * n + 1) * LANES, LANES)
        both = pl.ds(2 * n * LANES, 2 * LANES)
        cosine = low_ref[:, re]
        minus_sine = low_ref[:, im]
        high_ref[:, re] = cosine * keep + minus_sine * swap
        high_ref[:, im] = minus_sine * keep - cosine * swap
        spec_ref[:, both] = forward(filt, low_ref, high_ref, both, half)


def filter_spectrum_dense(filt):
    channels, length = filt.shape
    low = half_matrix(length)
    high, spec = call(
        filter_kernel,
        None,
        [
            jax.ShapeDtypeStruct((length // 2, 2 * length), bf16),
            jax.ShapeDtypeStruct((channels, 2 * length), f32),
        ],
        [],
        4 * channels * length * length,
        4 * channels * length * 3 + 4 * length * length,
        VMEM_MIB,
        (filt, low),
    )
    return (low, high), spec


def forward(rows, low_ref, high_ref, cols, half):
    low = jnp.dot(rows[:, :half], low_ref[:, cols], preferred_element_type=f32)
    return low + jnp.dot(rows[:, half:], high_ref[:, cols], preferred_element_type=f32)


def inverse(prod_ref, low_ref, high_ref, start, size):
    half = low_ref.shape[0]
    ref, start = (low_ref, start) if start < half else (high_ref, start - half)
    return lax.dot_general(
        prod_ref[...],
        ref[start : start + size, :],
        (((1,), (1,)), ((), ())),
        preferred_element_type=f32,
    ).astype(bf16)


def multiply_spectra(a_re, a_im, b_re, b_im, first_tile, length):
    rr = a_re * b_re
    ii = a_im * b_im
    cross = a_im * b_re - a_re * b_im
    if not first_tile:
        return (rr + ii) * (1.0 / length), cross * (1.0 / length)
    first = lax.broadcasted_iota(jnp.int32, rr.shape, 1) == 0
    scale = jnp.where(first, 0.5 / length, 1.0 / length)
    return jnp.where(first, rr, rr + ii) * scale, jnp.where(first, ii, cross) * scale


def gather_rows(axis, which, got_refs, rows_ref):
    me = lax.axis_index(axis)
    for k, got_ref in enumerate(got_refs):
        rows_ref[me ^ k] = got_ref[...] if len(got_ref.shape) == 2 else got_ref[which]
    return jnp.concatenate([rows_ref[p] for p in range(len(got_refs))], axis=1)


def correlate_kernel(axis, low_ref, high_ref, filt_spec_ref, *refs):
    count = (len(refs) - 3) // 2
    got_refs, out_refs = refs[:count], refs[count : 2 * count]
    spec_ref, rows_ref, prod_ref = refs[2 * count :]
    block = rows_ref.shape[2]
    length = count * block
    rows = gather_rows(axis, 0, got_refs, rows_ref)
    for n in range(length // LANES):
        re = pl.ds(2 * n * LANES, LANES)
        im = pl.ds((2 * n + 1) * LANES, LANES)
        both = pl.ds(2 * n * LANES, 2 * LANES)
        spec = forward(rows, low_ref, high_ref, both, length // 2)
        spec_ref[:, both] = spec
        real, imag = multiply_spectra(
            spec[:, :LANES], spec[:, LANES:], filt_spec_ref[:, re], filt_spec_ref[:, im], n == 0, length
        )
        prod_ref[:, re] = real.astype(bf16)
        prod_ref[:, im] = imag.astype(bf16)
    pair = 2 * LANES // block
    for q in range(count // pair):
        out = inverse(prod_ref, low_ref, high_ref, q * 2 * LANES, 2 * LANES)
        for part in range(pair):
            rows_ref[q * pair + part] = out[:, part * block : (part + 1) * block]
    me = lax.axis_index(axis)
    for k, out_ref in enumerate(out_refs):
        out_ref[...] = rows_ref[me ^ k]


def correlate_dense(got, w, filt_spec, axis):
    count = len(got)
    channels, block = got[-1].shape
    length = count * block
    *corr, spec = call(
        functools.partial(correlate_kernel, axis),
        None,
        [jax.ShapeDtypeStruct((channels, block), bf16)] * count
        + [jax.ShapeDtypeStruct((channels, 2 * length), f32)],
        [pltpu.VMEM((count, channels, block), bf16), pltpu.VMEM((channels, 2 * length), bf16)],
        8 * channels * length * length,
        4 * length * length + 20 * channels * length,
        VMEM_MIB,
        (*w, filt_spec, *got),
    )
    return corr, spec


def gradient_kernel(axis, share_axis, shares, low_ref, high_ref, grad_spec_ref, *refs):
    count = len(refs) - shares - 3
    got_refs, out_refs = refs[:count], refs[count : count + shares]
    rows_ref, prod_ref, taps_ref = refs[count + shares :]
    length = count * rows_ref.shape[2]
    rows = gather_rows(axis, 1, got_refs, rows_ref)
    for n in range(length // LANES):
        re = pl.ds(2 * n * LANES, LANES)
        im = pl.ds((2 * n + 1) * LANES, LANES)
        both = pl.ds(2 * n * LANES, 2 * LANES)
        spec = forward(rows, low_ref, high_ref, both, length // 2)
        real, imag = multiply_spectra(
            grad_spec_ref[:, re], grad_spec_ref[:, im], spec[:, :LANES], spec[:, LANES:], n == 0, length
        )
        prod_ref[:, re] = real.astype(bf16)
        prod_ref[:, im] = imag.astype(bf16)
    taps = length // shares
    for q in range(shares):
        taps_ref[q] = inverse(prod_ref, low_ref, high_ref, q * taps, taps)
    me = lax.axis_index(share_axis)
    for k, out_ref in enumerate(out_refs):
        out_ref[...] = taps_ref[me ^ k]


def gradient_dense(got, w, grad_spec, axis, share_axis):
    count = len(got)
    shares = lax.axis_size(share_axis)
    channels, block = got[-1].shape
    length = count * block
    return call(
        functools.partial(gradient_kernel, axis, share_axis, shares),
        None,
        [jax.ShapeDtypeStruct((channels, length // shares), bf16)] * shares,
        [
            pltpu.VMEM((count, channels, block), bf16),
            pltpu.VMEM((channels, 2 * length), bf16),
            pltpu.VMEM((shares, channels, length // shares), bf16),
        ],
        8 * channels * length * length,
        4 * length * length + 20 * channels * length,
        VMEM_MIB,
        (*w, grad_spec, *got),
    )


def finish_kernel(axis, shares, scale, base_ref, pr_ref, vb_ref, *refs):
    count = len(refs) - shares - 7
    back_refs, term_refs = refs[:count], refs[count : count + shares]
    pre_out, value_out, grad_out, pre_buf, value_buf, grad_buf, sems = refs[count + shares :]
    rows = back_refs[0].shape[0]
    copies = []

    def send(source, target, sem):
        copy = pltpu.make_async_copy(source, target, sem)
        copy.start()
        copies.append(copy)

    for k, back_ref in enumerate(back_refs):
        block = peer_rows(axis, k, rows)
        summed = back_ref[...].astype(f32) + base_ref[block]
        pre_buf[k] = (summed * vb_ref[block].astype(f32)).astype(bf16)
        value_buf[k] = (summed * pr_ref[block].astype(f32)).astype(bf16)
        send(pre_buf.at[k], pre_out.at[block], sems.at[0, k])
        send(value_buf.at[k], value_out.at[block], sems.at[1, k])
    grad_buf[...] = sum(term_ref[...].astype(f32) for term_ref in term_refs) * scale
    send(grad_buf, grad_out, sems.at[2, 0])
    for copy in copies:
        copy.wait()


def finish(back, base, pre_gate, value_branch, terms, scale, axis):
    count = len(back)
    rows, block = back[0].shape
    channels = count * rows
    return call(
        functools.partial(finish_kernel, axis, len(terms), scale),
        [pl.BlockSpec(memory_space=pltpu.HBM)] * 3,
        [jax.ShapeDtypeStruct((channels, block), bf16)] * 2
        + [jax.ShapeDtypeStruct(terms[0].shape, f32)],
        [
            pltpu.VMEM((count, rows, block), bf16),
            pltpu.VMEM((count, rows, block), bf16),
            pltpu.VMEM(terms[0].shape, f32),
            pltpu.SemaphoreType.DMA((3, count)),
        ],
        3 * channels * block,
        14 * channels * block,
        8,
        (base, pre_gate, value_branch, *back, *terms),
    )


def swap(value, axis, k):
    return lax.ppermute(value, axis, [(j, j ^ k) for j in range(lax.axis_size(axis))])


def peers(count):
    return list(range(count // 2)), list(range(count // 2, count))


def shards_dense(grad_output, post_gate, pre_gate, value_branch, long_filter, skip_weight):
    groups = lax.axis_size("ctx")
    shares = lax.axis_size("dp")
    seqs, channels, block = grad_output.shape
    length = long_filter.shape[1]
    token_count = seqs * shares * length
    near, far = peers(groups)
    rows = [x.reshape(channels, block) for x in (grad_output, post_gate, pre_gate, value_branch)]
    both, gated, saved = product(rows, near, far, "ctx")
    gated = [swap(gated[k], "ctx", k) for k in far]
    both = [both[0]] + [swap(both[k], "ctx", k) for k in near[1:]]
    saved = [swap(saved[k], "ctx", k) for k in far]
    w, filt_spec = filter_spectrum_dense(long_filter)
    own = (rows[0].astype(f32) * rows[1].astype(f32)).astype(bf16)
    base = skip_weight[:, None] * own.astype(f32)
    corr, grad_spec = correlate_dense(both + gated, w, filt_spec, "ctx")
    back = corr[:1] + [swap(corr[k], "ctx", k) for k in range(1, groups)]
    terms = gradient_dense(both + saved, w, grad_spec, "ctx", "dp")
    terms = terms[:1] + [swap(terms[k], "dp", k) for k in range(1, shares)]
    grad_pre_gate, grad_value_branch, grad_long_filter = finish(
        back, base, rows[2], rows[3], terms, 1.0 / math.sqrt(token_count), "ctx"
    )
    shape = grad_output.shape
    return (grad_pre_gate.reshape(shape), grad_value_branch.reshape(shape), grad_long_filter)


def split_factor(length):
    for candidate in range(128, 1, -1):
        if length % candidate == 0:
            return candidate
    return 1


def twiddle(row_count, col_count, modulus, sign_value):
    row_index = lax.broadcasted_iota(jnp.int32, (row_count, col_count), 0)
    col_index = lax.broadcasted_iota(jnp.int32, (row_count, col_count), 1)
    phases = row_index * col_index % modulus
    angles = phases.astype(jnp.float32) * (2.0 * math.pi / modulus)
    return (jnp.cos(angles), sign_value * jnp.sin(angles))


def block_matrix(row_count, col_count, modulus, sign_value, part_count):
    cosine, sine = twiddle(row_count, col_count, modulus, sign_value)
    matrix = jnp.stack([jnp.stack([cosine, sine], 1), jnp.stack([-sine, cosine], 1)], 0)
    return matrix[:part_count]


def transform(parts, sign_value, length):
    part_count = parts.shape[0]
    width = parts.shape[-1]
    leading = split_factor(length)
    if length <= 256 or leading == 1 or leading == length:
        matrix = block_matrix(width, length, length, sign_value, part_count)
        return jnp.einsum("p...j,pjqk->q...k", parts, matrix, precision=highest)
    trailing = length // leading
    live = -(-width // trailing)
    if live * trailing != width:
        extra = [(0, 0)] * (parts.ndim - 1) + [(0, live * trailing - width)]
        parts = jnp.pad(parts, extra)
    batch_dims = parts.shape[1:-1]
    parts = parts.reshape((part_count,) + batch_dims + (live, trailing))
    matrix = block_matrix(live, leading, leading, sign_value, part_count)
    first = jnp.einsum("p...jb,pjqk->q...kb", parts, matrix, precision=highest)
    turn_cos, turn_sin = twiddle(leading, trailing, length, sign_value)
    rotated = jnp.stack(
        [first[0] * turn_cos - first[1] * turn_sin, first[0] * turn_sin + first[1] * turn_cos], 0
    )
    deep = transform(rotated, sign_value, trailing)
    return jnp.swapaxes(deep, -1, -2).reshape((2,) + batch_dims + (length,))


def mirror(values):
    return jnp.roll(jnp.flip(values, -1), 1, -1)


def filter_spectrum(filter_rows):
    length = filter_rows.shape[1]
    spectrum = transform(filter_rows[None], -1.0, 2 * length)
    return (spectrum[0], spectrum[1])


def correlate(grad_rows, saved_rows, filt_real, filt_imag):
    length = grad_rows.shape[2]
    padded = 2 * length
    stacked = jnp.stack([grad_rows.astype(jnp.float32), saved_rows.astype(jnp.float32)], 0)
    spectrum = transform(stacked, -1.0, padded)
    spec_real = spectrum[0]
    spec_imag = spectrum[1]
    flip_real = mirror(spec_real)
    flip_imag = mirror(spec_imag)
    grad_real = 0.5 * (spec_real + flip_real)
    grad_imag = 0.5 * (spec_imag - flip_imag)
    input_real = 0.5 * (spec_imag + flip_imag)
    input_imag = 0.5 * (flip_real - spec_real)
    first_real = filt_real * grad_real + filt_imag * grad_imag
    first_imag = filt_real * grad_imag - filt_imag * grad_real
    second_real = grad_real * input_real + grad_imag * input_imag
    second_imag = grad_imag * input_real - grad_real * input_imag
    combined = jnp.stack([first_real - second_imag, first_imag + second_real], 0)
    result = transform(combined, 1.0, padded)
    factor = 1.0 / padded
    correlated = (result[0, ..., :length] * factor).astype(jnp.bfloat16)
    filter_terms = result[1, ..., :length] * factor
    return (correlated, filter_terms)


def shards_long(grad_output, post_gate, pre_gate, value_branch, long_filter, skip_weight):
    seq_count = grad_output.shape[0]
    length = long_filter.shape[1]
    token_count = seq_count * lax.axis_size("dp") * length
    gated = (grad_output.astype(jnp.float32) * post_gate.astype(jnp.float32)).astype(jnp.bfloat16)
    saved = (pre_gate.astype(jnp.float32) * value_branch.astype(jnp.float32)).astype(jnp.bfloat16)
    filt_real, filt_imag = filter_spectrum(long_filter)
    correlated, filter_terms = correlate(
        lax.all_to_all(gated, "ctx", split_axis=1, concat_axis=2, tiled=True),
        lax.all_to_all(saved, "ctx", split_axis=1, concat_axis=2, tiled=True),
        filt_real,
        filt_imag,
    )
    back = lax.all_to_all(correlated, "ctx", split_axis=2, concat_axis=1, tiled=True)
    returned, filter_terms = (back, filter_terms)
    filter_sum = jnp.sum(filter_terms, axis=0)
    shares = lax.psum_scatter(
        filter_sum.astype(jnp.bfloat16), "dp", scatter_dimension=1, tiled=True
    ).astype(jnp.float32)
    summed = returned.astype(jnp.float32) + skip_weight[None, :, None] * gated.astype(jnp.float32)
    grad_pre_gate = (summed * value_branch.astype(jnp.float32)).astype(jnp.bfloat16)
    grad_value_branch = (summed * pre_gate.astype(jnp.float32)).astype(jnp.bfloat16)
    grad_long_filter = shares * (1.0 / math.sqrt(token_count))
    return (grad_pre_gate, grad_value_branch, grad_long_filter)


def shards(grad_output, post_gate, pre_gate, value_branch, long_filter, skip_weight):
    seqs, _, block = grad_output.shape
    rows, length = long_filter.shape
    groups = lax.axis_size("ctx")
    shares = lax.axis_size("dp")
    dense = (
        seqs == 1
        and length <= 1024
        and block == LANES
        and rows % 16 == 0
        and length % (2 * LANES * shares) == 0
        and length % (4 * LANES) == 0
        and groups & (groups - 1) == 0
        and shares & (shares - 1) == 0
        and groups > 2
    )
    body = shards_dense if dense else shards_long
    return body(grad_output, post_gate, pre_gate, value_branch, long_filter, skip_weight)


def solution(mesh):
    return jax.shard_map(
        shards,
        mesh=mesh,
        in_specs=(
            P("dp", None, "ctx"),
            P("dp", None, "ctx"),
            P("dp", None, "ctx"),
            P("dp", None, "ctx"),
            P("ctx", None),
            P(),
        ),
        out_specs=(P("dp", None, "ctx"), P("dp", None, "ctx"), P("ctx", "dp")),
        check_vma=False,
    )
```

```python
import functools
import math

import jax
import jax.numpy as jnp
import numpy as np
from jax import lax
from jax.experimental import pallas as pl
from jax.experimental.pallas import tpu as pltpu
from jax.sharding import PartitionSpec as P


highest = lax.Precision.HIGHEST
f32 = jnp.float32
bf16 = jnp.bfloat16
LANES = 128
VMEM_MIB = 12


def half_matrix(length):
    time = np.arange(length // 2)[:, None]
    phase = (time * np.arange(length)[None, :] % (2 * length)) * (math.pi / length)
    pair = np.stack([np.cos(phase), -np.sin(phase)], axis=1)
    pair[:, 1, 0] = 1.0 - 2.0 * (time[:, 0] % 2)
    tiles = pair.reshape(length // 2, 2, length // LANES, LANES).transpose(0, 2, 1, 3)
    return jnp.asarray(tiles.reshape(length // 2, 2 * length), bf16)


def in_hbm(*arrays):
    return [pltpu.with_memory_space_constraint(array, pltpu.HBM) for array in arrays]


def peer_rows(axis, k, rows):
    return pl.ds(pl.multiple_of((lax.axis_index(axis) ^ k) * rows, rows), rows)


def call(kernel, out_specs, out_shape, scratch, flops, moved, mib, operands, in_specs=None):
    vmem = pl.BlockSpec(memory_space=pltpu.VMEM)
    return list(pl.pallas_call(
        kernel,
        in_specs=in_specs or [vmem] * len(operands),
        out_specs=out_specs or [vmem] * len(out_shape),
        out_shape=out_shape,
        scratch_shapes=scratch,
        compiler_params=pltpu.CompilerParams(vmem_limit_bytes=mib * 2**20),
        cost_estimate=pl.CostEstimate(flops=flops, bytes_accessed=moved, transcendentals=0),
    )(*operands))


def product_kernel(axis, plan, *refs):
    count = 2 * (1 + max(pair for _, pair, _ in plan))
    in_refs, out_refs = refs[:count], refs[count:-2]
    buf_ref, sems = refs[-2:]
    rows = buf_ref.shape[2]
    copies = []
    for i, (k, pair, _) in enumerate(plan):
        copies.append(
            [
                pltpu.make_async_copy(
                    in_refs[2 * pair + j].at[peer_rows(axis, k, rows)], buf_ref.at[j, i], sems.at[j, i]
                )
                for j in range(2)
            ]
        )
        for copy in copies[i]:
            copy.start()
    for i, (_, _, (at, slot)) in enumerate(plan):
        for copy in copies[i]:
            copy.wait()
        value = (buf_ref[0, i].astype(f32) * buf_ref[1, i].astype(f32)).astype(bf16)
        if slot is None:
            out_refs[at][...] = value
        else:
            out_refs[at][slot] = value


def product(arrays, plan, slots, count, axis):
    channels, block = arrays[0].shape
    rows = channels // count
    return call(
        functools.partial(product_kernel, axis, plan),
        None,
        [jax.ShapeDtypeStruct(((n,) if n > 1 else ()) + (rows, block), bf16) for n in slots],
        [pltpu.VMEM((2, len(plan), rows, block), bf16), pltpu.SemaphoreType.DMA((2, len(plan)))],
        len(plan) * rows * block,
        6 * len(plan) * rows * block,
        4,
        in_hbm(*arrays),
        [pl.BlockSpec(memory_space=pltpu.HBM)] * len(arrays),
    )


def filter_kernel(filt_ref, low_ref, high_ref, spec_ref):
    length = filt_ref.shape[1]
    half = length // 2
    filt = filt_ref[...].astype(bf16)
    turn = lax.broadcasted_iota(jnp.int32, (1, LANES), 1) % 4
    keep = jnp.where(turn == 0, 1.0, jnp.where(turn == 2, -1.0, 0.0)).astype(bf16)
    swap = jnp.where(turn == 1, 1.0, jnp.where(turn == 3, -1.0, 0.0)).astype(bf16)
    for n in range(length // LANES):
        re = pl.ds(2 * n * LANES, LANES)
        im = pl.ds((2 * n + 1) * LANES, LANES)
        both = pl.ds(2 * n * LANES, 2 * LANES)
        cosine = low_ref[:, re]
        minus_sine = low_ref[:, im]
        high_ref[:, re] = cosine * keep + minus_sine * swap
        high_ref[:, im] = minus_sine * keep - cosine * swap
        spec_ref[:, both] = forward(filt, low_ref, high_ref, both, half)


def filter_spectrum_dense(filt):
    channels, length = filt.shape
    low = half_matrix(length)
    high, spec = call(
        filter_kernel,
        None,
        [
            jax.ShapeDtypeStruct((length // 2, 2 * length), bf16),
            jax.ShapeDtypeStruct((channels, 2 * length), f32),
        ],
        [],
        4 * channels * length * length,
        4 * channels * length * 3 + 4 * length * length,
        VMEM_MIB,
        (filt, low),
    )
    return (low, high), spec


def forward(rows, low_ref, high_ref, cols, half):
    low = jnp.dot(rows[:, :half], low_ref[:, cols], preferred_element_type=f32)
    return low + jnp.dot(rows[:, half:], high_ref[:, cols], preferred_element_type=f32)


def inverse(prod_ref, low_ref, high_ref, start, size):
    half = low_ref.shape[0]
    ref, start = (low_ref, start) if start < half else (high_ref, start - half)
    return lax.dot_general(
        prod_ref[...],
        ref[start : start + size, :],
        (((1,), (1,)), ((), ())),
        preferred_element_type=f32,
    ).astype(bf16)


def multiply_spectra(a_re, a_im, b_re, b_im, first_tile, length):
    rr = a_re * b_re
    ii = a_im * b_im
    cross = a_im * b_re - a_re * b_im
    if not first_tile:
        return (rr + ii) * (1.0 / length), cross * (1.0 / length)
    first = lax.broadcasted_iota(jnp.int32, rr.shape, 1) == 0
    scale = jnp.where(first, 0.5 / length, 1.0 / length)
    return jnp.where(first, rr, rr + ii) * scale, jnp.where(first, ii, cross) * scale


def gather_rows(axis, which, got_refs, rows_ref):
    me = lax.axis_index(axis)
    for k, got_ref in enumerate(got_refs):
        rows_ref[me ^ k] = got_ref[...] if len(got_ref.shape) == 2 else got_ref[which]
    return jnp.concatenate([rows_ref[p] for p in range(len(got_refs))], axis=1)


def correlate_kernel(axis, low_ref, high_ref, filt_spec_ref, *refs):
    count = (len(refs) - 3) // 2
    got_refs, out_refs = refs[:count], refs[count : 2 * count]
    spec_ref, rows_ref, prod_ref = refs[2 * count :]
    block = rows_ref.shape[2]
    length = count * block
    rows = gather_rows(axis, 0, got_refs, rows_ref)
    for n in range(length // LANES):
        re = pl.ds(2 * n * LANES, LANES)
        im = pl.ds((2 * n + 1) * LANES, LANES)
        both = pl.ds(2 * n * LANES, 2 * LANES)
        spec = forward(rows, low_ref, high_ref, both, length // 2)
        spec_ref[:, both] = spec
        real, imag = multiply_spectra(
            spec[:, :LANES], spec[:, LANES:], filt_spec_ref[:, re], filt_spec_ref[:, im], n == 0, length
        )
        prod_ref[:, re] = real.astype(bf16)
        prod_ref[:, im] = imag.astype(bf16)
    pair = 2 * LANES // block
    for q in range(count // pair):
        out = inverse(prod_ref, low_ref, high_ref, q * 2 * LANES, 2 * LANES)
        for part in range(pair):
            rows_ref[q * pair + part] = out[:, part * block : (part + 1) * block]
    me = lax.axis_index(axis)
    for k, out_ref in enumerate(out_refs):
        out_ref[...] = rows_ref[me ^ k]


def correlate_dense(got, w, filt_spec, axis):
    count = len(got)
    channels, block = got[-1].shape
    length = count * block
    *corr, spec = call(
        functools.partial(correlate_kernel, axis),
        None,
        [jax.ShapeDtypeStruct((channels, block), bf16)] * count
        + [jax.ShapeDtypeStruct((channels, 2 * length), f32)],
        [pltpu.VMEM((count, channels, block), bf16), pltpu.VMEM((channels, 2 * length), bf16)],
        8 * channels * length * length,
        4 * length * length + 20 * channels * length,
        VMEM_MIB,
        (*w, filt_spec, *got),
    )
    return corr, spec


def gradient_kernel(axis, share_axis, shares, low_ref, high_ref, grad_spec_ref, *refs):
    count = len(refs) - shares - 3
    got_refs, out_refs = refs[:count], refs[count : count + shares]
    rows_ref, prod_ref, taps_ref = refs[count + shares :]
    length = count * rows_ref.shape[2]
    rows = gather_rows(axis, 1, got_refs, rows_ref)
    for n in range(length // LANES):
        re = pl.ds(2 * n * LANES, LANES)
        im = pl.ds((2 * n + 1) * LANES, LANES)
        both = pl.ds(2 * n * LANES, 2 * LANES)
        spec = forward(rows, low_ref, high_ref, both, length // 2)
        real, imag = multiply_spectra(
            grad_spec_ref[:, re], grad_spec_ref[:, im], spec[:, :LANES], spec[:, LANES:], n == 0, length
        )
        prod_ref[:, re] = real.astype(bf16)
        prod_ref[:, im] = imag.astype(bf16)
    taps = length // shares
    for q in range(shares):
        taps_ref[q] = inverse(prod_ref, low_ref, high_ref, q * taps, taps)
    me = lax.axis_index(share_axis)
    for k, out_ref in enumerate(out_refs):
        out_ref[...] = taps_ref[me ^ k]


def gradient_dense(got, w, grad_spec, axis, share_axis):
    count = len(got)
    shares = lax.axis_size(share_axis)
    channels, block = got[-1].shape
    length = count * block
    return call(
        functools.partial(gradient_kernel, axis, share_axis, shares),
        None,
        [jax.ShapeDtypeStruct((channels, length // shares), bf16)] * shares,
        [
            pltpu.VMEM((count, channels, block), bf16),
            pltpu.VMEM((channels, 2 * length), bf16),
            pltpu.VMEM((shares, channels, length // shares), bf16),
        ],
        8 * channels * length * length,
        4 * length * length + 20 * channels * length,
        VMEM_MIB,
        (*w, grad_spec, *got),
    )


def finish_kernel(axis, shares, scale, base_ref, pr_ref, vb_ref, *refs):
    count = len(refs) - shares - 7
    back_refs, term_refs = refs[:count], refs[count : count + shares]
    pre_out, value_out, grad_out, pre_buf, value_buf, grad_buf, sems = refs[count + shares :]
    rows = back_refs[0].shape[0]
    copies = []

    def send(source, target, sem):
        copy = pltpu.make_async_copy(source, target, sem)
        copy.start()
        copies.append(copy)

    for k, back_ref in enumerate(back_refs):
        block = peer_rows(axis, k, rows)
        summed = back_ref[...].astype(f32) + base_ref[block]
        pre_buf[k] = (summed * vb_ref[block].astype(f32)).astype(bf16)
        value_buf[k] = (summed * pr_ref[block].astype(f32)).astype(bf16)
        send(pre_buf.at[k], pre_out.at[block], sems.at[0, k])
        send(value_buf.at[k], value_out.at[block], sems.at[1, k])
    grad_buf[...] = sum(term_ref[...].astype(f32) for term_ref in term_refs) * scale
    send(grad_buf, grad_out, sems.at[2, 0])
    for copy in copies:
        copy.wait()


def finish(back, base, pre_gate, value_branch, terms, scale, axis):
    count = len(back)
    rows, block = back[0].shape
    channels = count * rows
    return call(
        functools.partial(finish_kernel, axis, len(terms), scale),
        [pl.BlockSpec(memory_space=pltpu.HBM)] * 3,
        [jax.ShapeDtypeStruct((channels, block), bf16)] * 2
        + [jax.ShapeDtypeStruct(terms[0].shape, f32)],
        [
            pltpu.VMEM((count, rows, block), bf16),
            pltpu.VMEM((count, rows, block), bf16),
            pltpu.VMEM(terms[0].shape, f32),
            pltpu.SemaphoreType.DMA((3, count)),
        ],
        3 * channels * block,
        14 * channels * block,
        8,
        (base, pre_gate, value_branch, *back, *terms),
    )


def swap(value, axis, k):
    return lax.ppermute(value, axis, [(j, j ^ k) for j in range(lax.axis_size(axis))])


def peers(count):
    return list(range(count // 2)), list(range(count // 2, count))


def shards_dense(grad_output, post_gate, pre_gate, value_branch, long_filter, skip_weight):
    groups = lax.axis_size("ctx")
    shares = lax.axis_size("dp")
    seqs, channels, block = grad_output.shape
    length = long_filter.shape[1]
    token_count = seqs * shares * length
    near, far = peers(groups)
    rows = [x.reshape(channels, block) for x in (grad_output, post_gate, pre_gate, value_branch)]
    first = [(k, 0, (i, None)) for i, k in enumerate(far)]
    gated = product(rows[:2], first, [1] * len(far), groups, "ctx")
    gated = [swap(value, "ctx", k) for k, value in zip(far, gated)]
    rest = [(k, pair, (i, pair)) for i, k in enumerate(near[1:] + near[:1]) for pair in range(2)]
    rest += [(k, 1, (len(near) + i, None)) for i, k in enumerate(far)]
    out = product(rows, rest, [2] * len(near) + [1] * len(far), groups, "ctx")
    saved = [swap(value, "ctx", k) for k, value in zip(far, out[len(near) :])]
    both = [swap(value, "ctx", k) for k, value in zip(near[1:], out)]
    both = [out[len(near) - 1]] + both
    w, filt_spec = filter_spectrum_dense(long_filter)
    own = (rows[0].astype(f32) * rows[1].astype(f32)).astype(bf16)
    base = skip_weight[:, None] * own.astype(f32)
    corr, grad_spec = correlate_dense(both + gated, w, filt_spec, "ctx")
    back = corr[:1] + [swap(corr[k], "ctx", k) for k in range(1, groups)]
    terms = gradient_dense(both + saved, w, grad_spec, "ctx", "dp")
    terms = terms[:1] + [swap(terms[k], "dp", k) for k in range(1, shares)]
    grad_pre_gate, grad_value_branch, grad_long_filter = finish(
        back, base, rows[2], rows[3], terms, 1.0 / math.sqrt(token_count), "ctx"
    )
    shape = grad_output.shape
    return (grad_pre_gate.reshape(shape), grad_value_branch.reshape(shape), grad_long_filter)


def split_factor(length):
    for candidate in range(128, 1, -1):
        if length % candidate == 0:
            return candidate
    return 1


def twiddle(row_count, col_count, modulus, sign_value):
    row_index = lax.broadcasted_iota(jnp.int32, (row_count, col_count), 0)
    col_index = lax.broadcasted_iota(jnp.int32, (row_count, col_count), 1)
    phases = row_index * col_index % modulus
    angles = phases.astype(jnp.float32) * (2.0 * math.pi / modulus)
    return (jnp.cos(angles), sign_value * jnp.sin(angles))


def block_matrix(row_count, col_count, modulus, sign_value, part_count):
    cosine, sine = twiddle(row_count, col_count, modulus, sign_value)
    matrix = jnp.stack([jnp.stack([cosine, sine], 1), jnp.stack([-sine, cosine], 1)], 0)
    return matrix[:part_count]


def transform(parts, sign_value, length):
    part_count = parts.shape[0]
    width = parts.shape[-1]
    leading = split_factor(length)
    if length <= 256 or leading == 1 or leading == length:
        matrix = block_matrix(width, length, length, sign_value, part_count)
        return jnp.einsum("p...j,pjqk->q...k", parts, matrix, precision=highest)
    trailing = length // leading
    live = -(-width // trailing)
    if live * trailing != width:
        extra = [(0, 0)] * (parts.ndim - 1) + [(0, live * trailing - width)]
        parts = jnp.pad(parts, extra)
    batch_dims = parts.shape[1:-1]
    parts = parts.reshape((part_count,) + batch_dims + (live, trailing))
    matrix = block_matrix(live, leading, leading, sign_value, part_count)
    first = jnp.einsum("p...jb,pjqk->q...kb", parts, matrix, precision=highest)
    turn_cos, turn_sin = twiddle(leading, trailing, length, sign_value)
    rotated = jnp.stack(
        [first[0] * turn_cos - first[1] * turn_sin, first[0] * turn_sin + first[1] * turn_cos], 0
    )
    deep = transform(rotated, sign_value, trailing)
    return jnp.swapaxes(deep, -1, -2).reshape((2,) + batch_dims + (length,))


def mirror(values):
    return jnp.roll(jnp.flip(values, -1), 1, -1)


def filter_spectrum(filter_rows):
    length = filter_rows.shape[1]
    spectrum = transform(filter_rows[None], -1.0, 2 * length)
    return (spectrum[0], spectrum[1])


def correlate(grad_rows, saved_rows, filt_real, filt_imag):
    length = grad_rows.shape[2]
    padded = 2 * length
    stacked = jnp.stack([grad_rows.astype(jnp.float32), saved_rows.astype(jnp.float32)], 0)
    spectrum = transform(stacked, -1.0, padded)
    spec_real = spectrum[0]
    spec_imag = spectrum[1]
    flip_real = mirror(spec_real)
    flip_imag = mirror(spec_imag)
    grad_real = 0.5 * (spec_real + flip_real)
    grad_imag = 0.5 * (spec_imag - flip_imag)
    input_real = 0.5 * (spec_imag + flip_imag)
    input_imag = 0.5 * (flip_real - spec_real)
    first_real = filt_real * grad_real + filt_imag * grad_imag
    first_imag = filt_real * grad_imag - filt_imag * grad_real
    second_real = grad_real * input_real + grad_imag * input_imag
    second_imag = grad_imag * input_real - grad_real * input_imag
    combined = jnp.stack([first_real - second_imag, first_imag + second_real], 0)
    result = transform(combined, 1.0, padded)
    factor = 1.0 / padded
    correlated = (result[0, ..., :length] * factor).astype(jnp.bfloat16)
    filter_terms = result[1, ..., :length] * factor
    return (correlated, filter_terms)


def shards_long(grad_output, post_gate, pre_gate, value_branch, long_filter, skip_weight):
    seq_count = grad_output.shape[0]
    length = long_filter.shape[1]
    token_count = seq_count * lax.axis_size("dp") * length
    gated = (grad_output.astype(jnp.float32) * post_gate.astype(jnp.float32)).astype(jnp.bfloat16)
    saved = (pre_gate.astype(jnp.float32) * value_branch.astype(jnp.float32)).astype(jnp.bfloat16)
    filt_real, filt_imag = filter_spectrum(long_filter)
    correlated, filter_terms = correlate(
        lax.all_to_all(gated, "ctx", split_axis=1, concat_axis=2, tiled=True),
        lax.all_to_all(saved, "ctx", split_axis=1, concat_axis=2, tiled=True),
        filt_real,
        filt_imag,
    )
    back = lax.all_to_all(correlated, "ctx", split_axis=2, concat_axis=1, tiled=True)
    returned, filter_terms = (back, filter_terms)
    filter_sum = jnp.sum(filter_terms, axis=0)
    shares = lax.psum_scatter(
        filter_sum.astype(jnp.bfloat16), "dp", scatter_dimension=1, tiled=True
    ).astype(jnp.float32)
    summed = returned.astype(jnp.float32) + skip_weight[None, :, None] * gated.astype(jnp.float32)
    grad_pre_gate = (summed * value_branch.astype(jnp.float32)).astype(jnp.bfloat16)
    grad_value_branch = (summed * pre_gate.astype(jnp.float32)).astype(jnp.bfloat16)
    grad_long_filter = shares * (1.0 / math.sqrt(token_count))
    return (grad_pre_gate, grad_value_branch, grad_long_filter)


def shards(grad_output, post_gate, pre_gate, value_branch, long_filter, skip_weight):
    seqs, _, block = grad_output.shape
    rows, length = long_filter.shape
    groups = lax.axis_size("ctx")
    shares = lax.axis_size("dp")
    dense = (
        seqs == 1
        and length <= 1024
        and block == LANES
        and rows % 16 == 0
        and length % (2 * LANES * shares) == 0
        and length % (4 * LANES) == 0
        and groups & (groups - 1) == 0
        and shares & (shares - 1) == 0
        and groups > 2
    )
    body = shards_dense if dense else shards_long
    return body(grad_output, post_gate, pre_gate, value_branch, long_filter, skip_weight)


def solution(mesh):
    return jax.shard_map(
        shards,
        mesh=mesh,
        in_specs=(
            P("dp", None, "ctx"),
            P("dp", None, "ctx"),
            P("dp", None, "ctx"),
            P("dp", None, "ctx"),
            P("ctx", None),
            P(),
        ),
        out_specs=(P("dp", None, "ctx"), P("dp", None, "ctx"), P("ctx", "dp")),
        check_vma=False,
    )
```

```python
import functools
import math

import jax
import jax.numpy as jnp
import numpy as np
from jax import lax
from jax.experimental import pallas as pl
from jax.experimental.pallas import tpu as pltpu
from jax.sharding import PartitionSpec as P


highest = lax.Precision.HIGHEST
f32 = jnp.float32
bf16 = jnp.bfloat16
LANES = 128
VMEM_MIB = 12


def half_matrix(length):
    time = np.arange(length // 2)[:, None]
    phase = (time * np.arange(length)[None, :] % (2 * length)) * (math.pi / length)
    pair = np.stack([np.cos(phase), -np.sin(phase)], axis=1)
    pair[:, 1, 0] = 1.0 - 2.0 * (time[:, 0] % 2)
    tiles = pair.reshape(length // 2, 2, length // LANES, LANES).transpose(0, 2, 1, 3)
    return jnp.asarray(tiles.reshape(length // 2, 2 * length), bf16)


def in_hbm(*arrays):
    return [pltpu.with_memory_space_constraint(array, pltpu.HBM) for array in arrays]


def peer_rows(axis, k, rows):
    return pl.ds(pl.multiple_of((lax.axis_index(axis) ^ k) * rows, rows), rows)


def call(kernel, out_specs, out_shape, scratch, flops, moved, mib, operands, in_specs=None, aliases={}):
    vmem = pl.BlockSpec(memory_space=pltpu.VMEM)
    return list(pl.pallas_call(
        kernel,
        in_specs=in_specs or [vmem] * len(operands),
        out_specs=out_specs or [vmem] * len(out_shape),
        out_shape=out_shape,
        scratch_shapes=scratch,
        input_output_aliases=aliases,
        compiler_params=pltpu.CompilerParams(vmem_limit_bytes=mib * 2**20),
        cost_estimate=pl.CostEstimate(flops=flops, bytes_accessed=moved, transcendentals=0),
    )(*operands))


def product_kernel(axis, plan, *refs):
    count = 2 * (1 + max(pair for _, pair, _ in plan))
    in_refs, out_refs = refs[:count], refs[count:-2]
    buf_ref, sems = refs[-2:]
    rows = buf_ref.shape[2]
    copies = []
    for i, (k, pair, _) in enumerate(plan):
        copies.append(
            [
                pltpu.make_async_copy(
                    in_refs[2 * pair + j].at[peer_rows(axis, k, rows)], buf_ref.at[j, i], sems.at[j, i]
                )
                for j in range(2)
            ]
        )
        for copy in copies[i]:
            copy.start()
    for i, (_, _, (at, slot)) in enumerate(plan):
        for copy in copies[i]:
            copy.wait()
        value = (buf_ref[0, i].astype(f32) * buf_ref[1, i].astype(f32)).astype(bf16)
        if slot is None:
            out_refs[at][...] = value
        else:
            out_refs[at][slot] = value


def product(arrays, plan, slots, count, axis):
    channels, block = arrays[0].shape
    rows = channels // count
    return call(
        functools.partial(product_kernel, axis, plan),
        None,
        [jax.ShapeDtypeStruct(((n,) if n > 1 else ()) + (rows, block), bf16) for n in slots],
        [pltpu.VMEM((2, len(plan), rows, block), bf16), pltpu.SemaphoreType.DMA((2, len(plan)))],
        len(plan) * rows * block,
        6 * len(plan) * rows * block,
        4,
        in_hbm(*arrays),
        [pl.BlockSpec(memory_space=pltpu.HBM)] * len(arrays),
    )


def filter_kernel(filt_ref, low_ref, high_ref, spec_ref):
    length = filt_ref.shape[1]
    half = length // 2
    filt = filt_ref[...].astype(bf16)
    turn = lax.broadcasted_iota(jnp.int32, (1, LANES), 1) % 4
    keep = jnp.where(turn == 0, 1.0, jnp.where(turn == 2, -1.0, 0.0)).astype(bf16)
    swap = jnp.where(turn == 1, 1.0, jnp.where(turn == 3, -1.0, 0.0)).astype(bf16)
    for n in range(length // LANES):
        re = pl.ds(2 * n * LANES, LANES)
        im = pl.ds((2 * n + 1) * LANES, LANES)
        both = pl.ds(2 * n * LANES, 2 * LANES)
        cosine = low_ref[:, re]
        minus_sine = low_ref[:, im]
        high_ref[:, re] = cosine * keep + minus_sine * swap
        high_ref[:, im] = minus_sine * keep - cosine * swap
        spec_ref[:, both] = forward(filt, low_ref, high_ref, both, half)


def filter_spectrum_dense(filt):
    channels, length = filt.shape
    low = half_matrix(length)
    high, spec = call(
        filter_kernel,
        None,
        [
            jax.ShapeDtypeStruct((length // 2, 2 * length), bf16),
            jax.ShapeDtypeStruct((channels, 2 * length), f32),
        ],
        [],
        4 * channels * length * length,
        4 * channels * length * 3 + 4 * length * length,
        VMEM_MIB,
        (filt, low),
    )
    return (low, high), spec


def forward(rows, low_ref, high_ref, cols, half):
    low = jnp.dot(rows[:, :half], low_ref[:, cols], preferred_element_type=f32)
    return low + jnp.dot(rows[:, half:], high_ref[:, cols], preferred_element_type=f32)


def inverse(prod_ref, low_ref, high_ref, start, size):
    half = low_ref.shape[0]
    ref, start = (low_ref, start) if start < half else (high_ref, start - half)
    return lax.dot_general(
        prod_ref[...],
        ref[start : start + size, :],
        (((1,), (1,)), ((), ())),
        preferred_element_type=f32,
    ).astype(bf16)


def multiply_spectra(a_re, a_im, b_re, b_im, first_tile, length):
    rr = a_re * b_re
    ii = a_im * b_im
    cross = a_im * b_re - a_re * b_im
    if not first_tile:
        return (rr + ii) * (1.0 / length), cross * (1.0 / length)
    first = lax.broadcasted_iota(jnp.int32, rr.shape, 1) == 0
    scale = jnp.where(first, 0.5 / length, 1.0 / length)
    return jnp.where(first, rr, rr + ii) * scale, jnp.where(first, ii, cross) * scale


def gather_rows(axis, which, got_refs, rows_ref):
    me = lax.axis_index(axis)
    for k, got_ref in enumerate(got_refs):
        rows_ref[me ^ k] = got_ref[...] if len(got_ref.shape) == 2 else got_ref[which]
    return jnp.concatenate([rows_ref[p] for p in range(len(got_refs))], axis=1)


def correlate_kernel(axis, low_ref, high_ref, filt_spec_ref, *refs):
    count = (len(refs) - 3) // 2
    got_refs, out_refs = refs[:count], refs[count : 2 * count]
    spec_ref, rows_ref, prod_ref = refs[2 * count :]
    block = rows_ref.shape[2]
    length = count * block
    rows = gather_rows(axis, 0, got_refs, rows_ref)
    for n in range(length // LANES):
        re = pl.ds(2 * n * LANES, LANES)
        im = pl.ds((2 * n + 1) * LANES, LANES)
        both = pl.ds(2 * n * LANES, 2 * LANES)
        spec = forward(rows, low_ref, high_ref, both, length // 2)
        spec_ref[:, both] = spec
        real, imag = multiply_spectra(
            spec[:, :LANES], spec[:, LANES:], filt_spec_ref[:, re], filt_spec_ref[:, im], n == 0, length
        )
        prod_ref[:, re] = real.astype(bf16)
        prod_ref[:, im] = imag.astype(bf16)
    pair = 2 * LANES // block
    for q in range(count // pair):
        out = inverse(prod_ref, low_ref, high_ref, q * 2 * LANES, 2 * LANES)
        for part in range(pair):
            rows_ref[q * pair + part] = out[:, part * block : (part + 1) * block]
    me = lax.axis_index(axis)
    for k, out_ref in enumerate(out_refs):
        out_ref[...] = rows_ref[me ^ k]


def correlate_dense(got, w, filt_spec, axis):
    count = len(got)
    channels, block = got[-1].shape
    length = count * block
    *corr, spec = call(
        functools.partial(correlate_kernel, axis),
        None,
        [jax.ShapeDtypeStruct((channels, block), bf16)] * count
        + [jax.ShapeDtypeStruct((channels, 2 * length), f32)],
        [pltpu.VMEM((count, channels, block), bf16), pltpu.VMEM((channels, 2 * length), bf16)],
        8 * channels * length * length,
        4 * length * length + 20 * channels * length,
        VMEM_MIB,
        (*w, filt_spec, *got),
    )
    return corr, spec


def gradient_kernel(axis, share_axis, shares, low_ref, high_ref, grad_spec_ref, *refs):
    count = len(refs) - shares - 3
    got_refs, out_refs = refs[:count], refs[count : count + shares]
    rows_ref, prod_ref, taps_ref = refs[count + shares :]
    length = count * rows_ref.shape[2]
    rows = gather_rows(axis, 1, got_refs, rows_ref)
    for n in range(length // LANES):
        re = pl.ds(2 * n * LANES, LANES)
        im = pl.ds((2 * n + 1) * LANES, LANES)
        both = pl.ds(2 * n * LANES, 2 * LANES)
        spec = forward(rows, low_ref, high_ref, both, length // 2)
        real, imag = multiply_spectra(
            grad_spec_ref[:, re], grad_spec_ref[:, im], spec[:, :LANES], spec[:, LANES:], n == 0, length
        )
        prod_ref[:, re] = real.astype(bf16)
        prod_ref[:, im] = imag.astype(bf16)
    taps = length // shares
    for q in range(shares):
        taps_ref[q] = inverse(prod_ref, low_ref, high_ref, q * taps, taps)
    me = lax.axis_index(share_axis)
    for k, out_ref in enumerate(out_refs):
        out_ref[...] = taps_ref[me ^ k]


def gradient_dense(got, w, grad_spec, axis, share_axis):
    count = len(got)
    shares = lax.axis_size(share_axis)
    channels, block = got[-1].shape
    length = count * block
    return call(
        functools.partial(gradient_kernel, axis, share_axis, shares),
        None,
        [jax.ShapeDtypeStruct((channels, length // shares), bf16)] * shares,
        [
            pltpu.VMEM((count, channels, block), bf16),
            pltpu.VMEM((channels, 2 * length), bf16),
            pltpu.VMEM((shares, channels, length // shares), bf16),
        ],
        8 * channels * length * length,
        4 * length * length + 20 * channels * length,
        VMEM_MIB,
        (*w, grad_spec, *got),
    )


def finish_kernel(axis, ks, held, scale, base_ref, pr_ref, vb_ref, *refs):
    refs = refs[held:]
    back_refs, refs = refs[: len(ks)], refs[len(ks) :]
    term_refs, refs = (refs[:-7], refs[-7:]) if held else ((), refs)
    pre_out, value_out, *grad, pre_buf, value_buf, sems = refs
    rows = pre_buf.shape[1]
    copies = []

    def send(source, target, sem):
        copy = pltpu.make_async_copy(source, target, sem)
        copy.start()
        copies.append(copy)

    for i, (k, back_ref) in enumerate(zip(ks, back_refs)):
        block = peer_rows(axis, k, rows)
        summed = back_ref[...].astype(f32) + base_ref[block]
        pre_buf[i] = (summed * vb_ref[block].astype(f32)).astype(bf16)
        value_buf[i] = (summed * pr_ref[block].astype(f32)).astype(bf16)
        send(pre_buf.at[i], pre_out.at[block], sems.at[0, i])
        send(value_buf.at[i], value_out.at[block], sems.at[1, i])
    if held:
        grad_out, grad_buf = grad
        grad_buf[...] = sum(term_ref[...].astype(f32) for term_ref in term_refs) * scale
        send(grad_buf, grad_out, sems.at[2, 0])
    for copy in copies:
        copy.wait()


def finish(back, ks, base, pre_gate, value_branch, axis, held=(), terms=(), scale=1.0):
    rows, block = back[0].shape
    channels = pre_gate.shape[0]
    vmem = pl.BlockSpec(memory_space=pltpu.VMEM)
    hbm = pl.BlockSpec(memory_space=pltpu.HBM)
    out_shape = [jax.ShapeDtypeStruct((channels, block), bf16)] * 2
    buffers = [pltpu.VMEM((len(ks), rows, block), bf16)] * 2
    if held:
        out_shape.append(jax.ShapeDtypeStruct(terms[0].shape, f32))
        buffers.insert(0, pltpu.VMEM(terms[0].shape, f32))
    return call(
        functools.partial(finish_kernel, axis, ks, len(held), scale),
        [hbm] * len(out_shape),
        out_shape,
        buffers + [pltpu.SemaphoreType.DMA((3, len(ks)))],
        3 * len(ks) * rows * block,
        14 * len(ks) * rows * block,
        8,
        (base, pre_gate, value_branch, *held, *back, *terms),
        [vmem] * 3 + [hbm] * len(held) + [vmem] * (len(back) + len(terms)),
        {3 + i: i for i in range(len(held))},
    )


def swap(value, axis, k):
    return lax.ppermute(value, axis, [(j, j ^ k) for j in range(lax.axis_size(axis))])


def peers(count):
    return list(range(count // 2)), list(range(count // 2, count))


def shards_dense(grad_output, post_gate, pre_gate, value_branch, long_filter, skip_weight):
    groups = lax.axis_size("ctx")
    shares = lax.axis_size("dp")
    seqs, channels, block = grad_output.shape
    length = long_filter.shape[1]
    token_count = seqs * shares * length
    near, far = peers(groups)
    rows = [x.reshape(channels, block) for x in (grad_output, post_gate, pre_gate, value_branch)]
    first = [(k, 0, (i, None)) for i, k in enumerate(far)]
    gated = product(rows[:2], first, [1] * len(far), groups, "ctx")
    gated = [swap(value, "ctx", k) for k, value in zip(far, gated)]
    rest = [(k, pair, (i, pair)) for i, k in enumerate(near[1:] + near[:1]) for pair in range(2)]
    rest += [(k, 1, (len(near) + i, None)) for i, k in enumerate(far)]
    out = product(rows, rest, [2] * len(near) + [1] * len(far), groups, "ctx")
    saved = [swap(value, "ctx", k) for k, value in zip(far, out[len(near) :])]
    both = [swap(value, "ctx", k) for k, value in zip(near[1:], out)]
    both = [out[len(near) - 1]] + both
    w, filt_spec = filter_spectrum_dense(long_filter)
    own = (rows[0].astype(f32) * rows[1].astype(f32)).astype(bf16)
    base = skip_weight[:, None] * own.astype(f32)
    corr, grad_spec = correlate_dense(both + gated, w, filt_spec, "ctx")
    back = corr[:1] + [swap(corr[k], "ctx", k) for k in range(1, groups)]
    terms = gradient_dense(both + saved, w, grad_spec, "ctx", "dp")
    terms = terms[:1] + [swap(terms[k], "dp", k) for k in range(1, shares)]
    early = near[:1] + far
    held = finish([back[k] for k in early], early, base, rows[2], rows[3], "ctx")
    grad_pre_gate, grad_value_branch, grad_long_filter = finish(
        [back[k] for k in near[1:]], near[1:], base, rows[2], rows[3], "ctx",
        held, terms, 1.0 / math.sqrt(token_count),
    )
    shape = grad_output.shape
    return (grad_pre_gate.reshape(shape), grad_value_branch.reshape(shape), grad_long_filter)


def split_factor(length):
    for candidate in range(128, 1, -1):
        if length % candidate == 0:
            return candidate
    return 1


def twiddle(row_count, col_count, modulus, sign_value):
    row_index = lax.broadcasted_iota(jnp.int32, (row_count, col_count), 0)
    col_index = lax.broadcasted_iota(jnp.int32, (row_count, col_count), 1)
    phases = row_index * col_index % modulus
    angles = phases.astype(jnp.float32) * (2.0 * math.pi / modulus)
    return (jnp.cos(angles), sign_value * jnp.sin(angles))


def block_matrix(row_count, col_count, modulus, sign_value, part_count):
    cosine, sine = twiddle(row_count, col_count, modulus, sign_value)
    matrix = jnp.stack([jnp.stack([cosine, sine], 1), jnp.stack([-sine, cosine], 1)], 0)
    return matrix[:part_count]


def transform(parts, sign_value, length):
    part_count = parts.shape[0]
    width = parts.shape[-1]
    leading = split_factor(length)
    if length <= 256 or leading == 1 or leading == length:
        matrix = block_matrix(width, length, length, sign_value, part_count)
        return jnp.einsum("p...j,pjqk->q...k", parts, matrix, precision=highest)
    trailing = length // leading
    live = -(-width // trailing)
    if live * trailing != width:
        extra = [(0, 0)] * (parts.ndim - 1) + [(0, live * trailing - width)]
        parts = jnp.pad(parts, extra)
    batch_dims = parts.shape[1:-1]
    parts = parts.reshape((part_count,) + batch_dims + (live, trailing))
    matrix = block_matrix(live, leading, leading, sign_value, part_count)
    first = jnp.einsum("p...jb,pjqk->q...kb", parts, matrix, precision=highest)
    turn_cos, turn_sin = twiddle(leading, trailing, length, sign_value)
    rotated = jnp.stack(
        [first[0] * turn_cos - first[1] * turn_sin, first[0] * turn_sin + first[1] * turn_cos], 0
    )
    deep = transform(rotated, sign_value, trailing)
    return jnp.swapaxes(deep, -1, -2).reshape((2,) + batch_dims + (length,))


def mirror(values):
    return jnp.roll(jnp.flip(values, -1), 1, -1)


def filter_spectrum(filter_rows):
    length = filter_rows.shape[1]
    spectrum = transform(filter_rows[None], -1.0, 2 * length)
    return (spectrum[0], spectrum[1])


def correlate(grad_rows, saved_rows, filt_real, filt_imag):
    length = grad_rows.shape[2]
    padded = 2 * length
    stacked = jnp.stack([grad_rows.astype(jnp.float32), saved_rows.astype(jnp.float32)], 0)
    spectrum = transform(stacked, -1.0, padded)
    spec_real = spectrum[0]
    spec_imag = spectrum[1]
    flip_real = mirror(spec_real)
    flip_imag = mirror(spec_imag)
    grad_real = 0.5 * (spec_real + flip_real)
    grad_imag = 0.5 * (spec_imag - flip_imag)
    input_real = 0.5 * (spec_imag + flip_imag)
    input_imag = 0.5 * (flip_real - spec_real)
    first_real = filt_real * grad_real + filt_imag * grad_imag
    first_imag = filt_real * grad_imag - filt_imag * grad_real
    second_real = grad_real * input_real + grad_imag * input_imag
    second_imag = grad_imag * input_real - grad_real * input_imag
    combined = jnp.stack([first_real - second_imag, first_imag + second_real], 0)
    result = transform(combined, 1.0, padded)
    factor = 1.0 / padded
    correlated = (result[0, ..., :length] * factor).astype(jnp.bfloat16)
    filter_terms = result[1, ..., :length] * factor
    return (correlated, filter_terms)


def shards_long(grad_output, post_gate, pre_gate, value_branch, long_filter, skip_weight):
    seq_count = grad_output.shape[0]
    length = long_filter.shape[1]
    token_count = seq_count * lax.axis_size("dp") * length
    gated = (grad_output.astype(jnp.float32) * post_gate.astype(jnp.float32)).astype(jnp.bfloat16)
    saved = (pre_gate.astype(jnp.float32) * value_branch.astype(jnp.float32)).astype(jnp.bfloat16)
    filt_real, filt_imag = filter_spectrum(long_filter)
    correlated, filter_terms = correlate(
        lax.all_to_all(gated, "ctx", split_axis=1, concat_axis=2, tiled=True),
        lax.all_to_all(saved, "ctx", split_axis=1, concat_axis=2, tiled=True),
        filt_real,
        filt_imag,
    )
    back = lax.all_to_all(correlated, "ctx", split_axis=2, concat_axis=1, tiled=True)
    returned, filter_terms = (back, filter_terms)
    filter_sum = jnp.sum(filter_terms, axis=0)
    shares = lax.psum_scatter(
        filter_sum.astype(jnp.bfloat16), "dp", scatter_dimension=1, tiled=True
    ).astype(jnp.float32)
    summed = returned.astype(jnp.float32) + skip_weight[None, :, None] * gated.astype(jnp.float32)
    grad_pre_gate = (summed * value_branch.astype(jnp.float32)).astype(jnp.bfloat16)
    grad_value_branch = (summed * pre_gate.astype(jnp.float32)).astype(jnp.bfloat16)
    grad_long_filter = shares * (1.0 / math.sqrt(token_count))
    return (grad_pre_gate, grad_value_branch, grad_long_filter)


def shards(grad_output, post_gate, pre_gate, value_branch, long_filter, skip_weight):
    seqs, _, block = grad_output.shape
    rows, length = long_filter.shape
    groups = lax.axis_size("ctx")
    shares = lax.axis_size("dp")
    dense = (
        seqs == 1
        and length <= 1024
        and block == LANES
        and rows % 16 == 0
        and length % (2 * LANES * shares) == 0
        and length % (4 * LANES) == 0
        and groups & (groups - 1) == 0
        and shares & (shares - 1) == 0
        and groups > 2
    )
    body = shards_dense if dense else shards_long
    return body(grad_output, post_gate, pre_gate, value_branch, long_filter, skip_weight)


def solution(mesh):
    return jax.shard_map(
        shards,
        mesh=mesh,
        in_specs=(
            P("dp", None, "ctx"),
            P("dp", None, "ctx"),
            P("dp", None, "ctx"),
            P("dp", None, "ctx"),
            P("ctx", None),
            P(),
        ),
        out_specs=(P("dp", None, "ctx"), P("dp", None, "ctx"), P("ctx", "dp")),
        check_vma=False,
    )
```
